256 devices in a mesh: section: 16 (over z, x_lo), fsdp: 16 (over x_hi, y, core).
Axes of the slice: x: 4 (x_hi: 2, x_lo: 2; x = x_hi * 2 + x_lo), y: 4, z: 8, core: 2. Of those that a mesh axis runs over, the one named last changes fastest.
Arguments:
- layer_inputs: bfloat16 [16, 2, 6144, 2048], P('section', None, 'fsdp'), may hold values from -6 to 6
- out_grads: bfloat16 [16, 2, 6144, 2048], P('section', None, 'fsdp'), may hold values from -6 to 6
- attn_stash: bfloat16 [16, 2, 6144, 1024], P('section', None, 'fsdp'), may hold values from -6 to 6
- proj_grads: bfloat16 [16, 2, 6144, 1536], P('section', None, 'fsdp'), may hold values from -6 to 6
- w_qkv: bfloat16 [16, 2048, 1536], P('section', 'fsdp'), may hold values from -0.125 to 0.125
- w_out: bfloat16 [16, 1024, 2048], P('section', 'fsdp'), may hold values from -0.1875 to 0.1875
- norm_gain: float32 [16, 2048], P('section'), may hold values from 0.25 to 1.75
- b_sched: int32 [16], P('section'), may hold values from 0 to 1
- w_sched: int32 [16], P('section'), may hold values from 0 to 1
Outputs:
- prev_grads: bfloat16 [16, 6144, 2048], P('section', 'fsdp')
- grad_qkv: float32 [16, 2048, 1536], P('section', 'fsdp')
- grad_out: float32 [16, 1024, 2048], P('section', 'fsdp')
The draws below stay inside these ranges and needn't reach their ends.
All inputs are finite; a program needn't handle non-finite values.
Results may differ from the reference program's by a relative error of at most 0.012.
Values may be sent and summed in bfloat16 or wider, within the bound.
No kernel may reach another device: no remote copies, remote signals or barrier semaphores. Data moves between devices by JAX's collectives and lax.ppermute only.
A program may use at most 128 MiB of HBM per device.

```python
import jax
import jax.numpy as jnp
from jax import lax

D = 2048
HEAD_DIM = 64
HEADS = 16
KV_HEADS = 4
SEQ = 384
MICRO = 2
SECTIONS = 16
Q_WIDTH = 1024
QKV_WIDTH = 1536
TOKENS = 6144
N_FSDP = 16


def set_ends(values, own_key, smallest, top_value):
    longest = values.shape.index(max(values.shape))
    spots = []
    for shift in (0, 1):
        where = [jax.random.randint(jax.random.fold_in(own_key, axis), (), 0, length) for axis, length in enumerate(values.shape)]
        where[longest] = (where[longest] + shift) % values.shape[longest]
        spots.append(tuple(where))
    return values.at[spots[0]].set(smallest).at[spots[1]].set(top_value)


def raised(values, stream_key, source, target, parts, factor):
    owner, partner = [(jnp.arange(values.shape[position]) // (values.shape[position] // parts)).reshape([-1 if axis == position else 1 for axis in range(values.ndim)]) for position in (source, target)]
    chosen = jax.random.permutation(stream_key, parts)[partner]
    strong = (owner == chosen) | (owner == (partner + parts // 2) % parts)
    return jnp.where(strong, factor * values, values)


def level_of(own_key, shape, cuts, smallest, high):
    def one(axis_at, blocks):
        steps = jax.random.uniform(jax.random.fold_in(jax.random.fold_in(own_key, 6), axis_at), (blocks,), jnp.float32, smallest / len(cuts), high / len(cuts))
        return jnp.repeat(jnp.exp(steps), shape[axis_at] // blocks).reshape((-1,) + (1,) * (len(shape) - axis_at - 1))

    loudness = one(*cuts[0])
    for cut in cuts[1:]:
        loudness = loudness * one(*cut)
    return loudness


def scatter_about(stream_key, dims, scale, bound, pieces=(), kind=jnp.bfloat16):
    loudness = level_of(stream_key, dims, pieces, -0.22, 0.18) if pieces else 1.0
    entries = jax.random.normal(stream_key, dims, jnp.float32) * scale * loudness
    return jnp.minimum(jnp.maximum(entries, -bound), bound).astype(kind)


def heavy_noise(key, dims, spread, most, pieces, heavy, kind=jnp.bfloat16):
    entries = spread * jax.random.normal(key, dims, jnp.float32)
    if pieces:
        entries = entries * level_of(key, dims, pieces, -0.22, 0.18)
    return jnp.clip(raised(entries, jax.random.fold_in(key, 3), *heavy), -most, most).astype(kind)


def setup_inputs(seed: int = 0) -> dict:
    streams_of = jax.random.split(jax.random.key(seed), 10)
    layer_inputs = scatter_about(streams_of[0], (SECTIONS, MICRO, TOKENS, D), 1.0, 6.0, ((0, 16), (2, 16)))
    out_grads = scatter_about(streams_of[1], (SECTIONS, MICRO, TOKENS, D), 1.0, 6.0, ((0, 16), (2, 16)))
    attn_stash = heavy_noise(streams_of[2], (SECTIONS, MICRO, TOKENS, Q_WIDTH), 1.0, 6.0, ((0, 16), (2, 16)), (2, 3, 16, 2.0))
    proj_grads = scatter_about(streams_of[3], (SECTIONS, MICRO, TOKENS, QKV_WIDTH), 1.0, 6.0, ((0, 16), (2, 16)))
    w_qkv = scatter_about(streams_of[4], (SECTIONS, D, QKV_WIDTH), D ** -0.5, 0.125, ((0, 16), (1, 16)))
    w_out = scatter_about(streams_of[5], (SECTIONS, Q_WIDTH, D), Q_WIDTH ** -0.5, 0.1875, ((0, 16), (1, 16)))
    norm_gain = jnp.clip(1.0 + 0.15 * jax.random.normal(streams_of[6], (SECTIONS, D), jnp.float32), 0.25, 1.75)
    b_sched = set_ends(jax.random.randint(streams_of[7], (SECTIONS,), 0, MICRO), jax.random.fold_in(streams_of[7], 1), 0, MICRO - 1).astype(jnp.int32)
    w_sched = set_ends(jax.random.randint(streams_of[8], (SECTIONS,), 0, MICRO), jax.random.fold_in(streams_of[8], 1), 0, MICRO - 1).astype(jnp.int32)
    return dict(layer_inputs=layer_inputs, out_grads=out_grads, attn_stash=attn_stash, proj_grads=proj_grads, w_qkv=w_qkv, w_out=w_out, norm_gain=norm_gain, b_sched=b_sched, w_sched=w_sched)


rms_eps = 1e-05
rope_base = 500000.0

def rope_tables(length, head_size):
    halfway = head_size // 2
    indices = jnp.arange(halfway, dtype=jnp.float32)
    frequency = rope_base ** (-2.0 * indices / head_size)
    angles = jnp.arange(length, dtype=jnp.float32)[:, None] * frequency[None, :]
    angles = jnp.concatenate([angles, angles], axis=1)
    return (jnp.cos(angles), jnp.sin(angles))

def rotate_half(values):
    halfway = values.shape[-1] // 2
    return jnp.concatenate([-values[..., halfway:], values[..., :halfway]], axis=-1)

def apply_rope(values, cosine_table, sine_table):
    return values * cosine_table[:, None, :] + rotate_half(values) * sine_table[:, None, :]

def unapply_rope(values, cosine_table, sine_table):
    return values * cosine_table[:, None, :] - rotate_half(values * sine_table[:, None, :])

def contract(pattern, first_operand, second_operand):
    return jnp.einsum(pattern, first_operand.astype(jnp.float32), second_operand.astype(jnp.float32))

def normalize(inputs, gain_values):
    widened = inputs.astype(jnp.float32)
    inv_rms = lax.rsqrt(lax.optimization_barrier(jnp.mean(widened * widened, axis=-1, keepdims=True)) + rms_eps)
    normed = (widened * inv_rms * gain_values).astype(jnp.bfloat16)
    return (widened, inv_rms, normed)

def attention_back(qkv_rows, attn_grad, cosine_table, sine_table):
    tokens_here = qkv_rows.shape[0]
    q_width = HEADS * HEAD_DIM
    kv_width = KV_HEADS * HEAD_DIM
    group_size = HEADS // KV_HEADS
    score_scale = HEAD_DIM ** (-0.5)
    queries = apply_rope(qkv_rows[:, :q_width].reshape(tokens_here, HEADS, HEAD_DIM), cosine_table, sine_table).astype(jnp.bfloat16)
    key_heads = apply_rope(qkv_rows[:, q_width:q_width + kv_width].reshape(tokens_here, KV_HEADS, HEAD_DIM), cosine_table, sine_table).astype(jnp.bfloat16)
    values = qkv_rows[:, q_width + kv_width:].reshape(tokens_here, KV_HEADS, HEAD_DIM).astype(jnp.bfloat16)
    queries = queries.reshape(tokens_here, KV_HEADS, group_size, HEAD_DIM)
    grad_heads = attn_grad.reshape(tokens_here, KV_HEADS, group_size, HEAD_DIM)
    scores = contract('tkgd,ukd->kgtu', queries, key_heads) * score_scale
    row_ids = lax.broadcasted_iota(jnp.int32, (tokens_here, tokens_here), 0)
    col_ids = lax.broadcasted_iota(jnp.int32, (tokens_here, tokens_here), 1)
    causal = col_ids <= row_ids
    exp_scores = jnp.where(causal, jnp.exp(scores), 0.0)
    attention = exp_scores / lax.optimization_barrier(jnp.sum(exp_scores, axis=-1, keepdims=True))
    attention_low = attention.astype(jnp.bfloat16)
    grad_values = contract('kgtu,tkgd->ukd', attention_low, grad_heads)
    grad_attention = contract('tkgd,ukd->kgtu', grad_heads, values)
    row_delta = lax.optimization_barrier(jnp.sum(attention * grad_attention, axis=-1, keepdims=True))
    grad_scores = (attention * (grad_attention - row_delta) * score_scale).astype(jnp.bfloat16)
    grad_queries = contract('kgtu,ukd->tkgd', grad_scores, key_heads)
    grad_keys = contract('kgtu,tkgd->ukd', grad_scores, queries)
    grad_queries = unapply_rope(grad_queries.reshape(tokens_here, HEADS, HEAD_DIM), cosine_table, sine_table)
    grad_keys = unapply_rope(grad_keys, cosine_table, sine_table)
    joined = jnp.concatenate([grad_queries.reshape(tokens_here, q_width), grad_keys.reshape(tokens_here, kv_width), grad_values.reshape(tokens_here, kv_width)], axis=1)
    return joined.astype(jnp.bfloat16)

def finish_grad(widened, inv_rms, gain_values, upstream, grad_normed):
    scaled = grad_normed * gain_values
    inner_mean = lax.optimization_barrier(jnp.mean(scaled * widened, axis=-1, keepdims=True))
    result = upstream.astype(jnp.float32) + inv_rms * scaled - widened * inv_rms ** 3 * inner_mean
    return result.astype(jnp.bfloat16)

def reference(layer_inputs, out_grads, attn_stash, proj_grads, w_qkv, w_out, norm_gain, b_sched, w_sched):
    cosine_table, sine_table = rope_tables(SEQ, HEAD_DIM)
    contract_rows = (((0,), (0,)), ((), ()))
    contract_cols = (((1,), (1,)), ((), ()))

    def one_section(operands):
        inputs, upstream, attended, projected, weight_qkv, weight_out, gain_values, b_slot, w_slot = operands
        inputs_b = lax.dynamic_index_in_dim(inputs, b_slot, 0, keepdims=False).reshape(N_FSDP, SEQ, D)
        upstream_b = lax.dynamic_index_in_dim(upstream, b_slot, 0, keepdims=False).reshape(N_FSDP, SEQ, D)

        def one_sequence(seq_pair):
            seq_inputs, seq_upstream = seq_pair
            widened, inv_rms, normed = normalize(seq_inputs, gain_values)
            qkv_rows = jnp.dot(normed, weight_qkv, preferred_element_type=jnp.float32)
            attn_grad = lax.dot_general(seq_upstream, weight_out, contract_cols, preferred_element_type=jnp.float32).astype(jnp.bfloat16)
            grad_proj = attention_back(qkv_rows, attn_grad, cosine_table, sine_table)
            grad_normed = lax.dot_general(grad_proj, weight_qkv, contract_cols, preferred_element_type=jnp.float32)
            return finish_grad(widened, inv_rms, gain_values, seq_upstream, grad_normed)
        sent_grads = lax.map(one_sequence, (inputs_b, upstream_b)).reshape(TOKENS, D)
        inputs_w = lax.dynamic_index_in_dim(inputs, w_slot, 0, keepdims=False).reshape(N_FSDP, SEQ, D)
        upstream_w = lax.dynamic_index_in_dim(upstream, w_slot, 0, keepdims=False).reshape(N_FSDP, SEQ, D)
        attended_w = lax.dynamic_index_in_dim(attended, w_slot, 0, keepdims=False).reshape(N_FSDP, SEQ, Q_WIDTH)
        projected_w = lax.dynamic_index_in_dim(projected, w_slot, 0, keepdims=False).reshape(N_FSDP, SEQ, QKV_WIDTH)

        def add_member(totals, member):
            m_inputs, m_upstream, m_attended, m_projected = member
            unused_wide, unused_inv, normed = normalize(m_inputs, gain_values)
            part_qkv = lax.dot_general(normed, m_projected, contract_rows, preferred_element_type=jnp.float32)
            part_out = lax.dot_general(m_attended, m_upstream, contract_rows, preferred_element_type=jnp.float32)
            part_qkv = lax.optimization_barrier(part_qkv.astype(jnp.bfloat16)).astype(jnp.float32)
            part_out = lax.optimization_barrier(part_out.astype(jnp.bfloat16)).astype(jnp.float32)
            return ((totals[0] + part_qkv, totals[1] + part_out), None)
        zero_totals = (jnp.zeros((D, QKV_WIDTH), jnp.float32), jnp.zeros((Q_WIDTH, D), jnp.float32))
        grad_pair, unused_out = lax.scan(add_member, zero_totals, (inputs_w, upstream_w, attended_w, projected_w))
        return (sent_grads, grad_pair[0], grad_pair[1])
    sent_all, grad_qkv, grad_out = lax.map(one_section, (layer_inputs, out_grads, attn_stash, proj_grads, w_qkv, w_out, norm_gain, b_sched, w_sched))
    return (jnp.roll(sent_all, -1, axis=0), grad_qkv, grad_out)
```

```python
import jax
import jax.numpy as jnp
from jax import lax
from jax.sharding import Mesh
from jax.sharding import PartitionSpec as P

HEAD_DIM = 64
HEADS = 16
KV_HEADS = 4
SECTION = ("z", "x_lo")
FSDP = ("x_hi", "y", "core")


rms_eps = 1e-05
rope_base = 500000.0


def passed_along(array, axis, by):
    size = lax.axis_size(axis)
    return lax.ppermute(array, axis, [(i, (i + by) % size) for i in range(size)])


def from_above(array):
    return passed_along(array, "y", -1)


def from_below(array):
    return passed_along(array, "y", 1)


def gathered_groups(shard):
    other = passed_along(shard, "x_hi", 1)
    above, below = (from_above(shard), from_below(shard))
    above_other, below_other = (from_above(other), from_below(other))
    far = from_above(above)
    far_other = from_below(below_other)
    pieces = {
        (0, 0): shard,
        (1, 0): other,
        (0, 1): above,
        (0, 3): below,
        (1, 1): above_other,
        (1, 3): below_other,
        (0, 2): far,
        (1, 2): far_other,
    }
    groups = []
    for keys in (((0, 0), (1, 0)), ((0, 1), (0, 3), (1, 1), (1, 3)), ((0, 2), (1, 2))):
        mine = jnp.stack([pieces[key] for key in keys])
        groups.append((keys, mine, passed_along(mine, "core", 1)))
    return groups


def assembled(shard):
    x_at, y_at, c_at = (lax.axis_index(name) for name in FSDP)
    rows = shard.shape[0]
    whole = jnp.zeros((16 * rows, shard.shape[1]), shard.dtype)
    for keys, mine, peers in gathered_groups(shard):
        for at, (dx, dy) in enumerate(keys):
            chip = (x_at ^ dx) * 8 + ((y_at + dy) % 4) * 2
            whole = lax.dynamic_update_slice(whole, mine[at], ((chip + c_at) * rows, 0))
            whole = lax.dynamic_update_slice(whole, peers[at], ((chip + 1 - c_at) * rows, 0))
    return whole


def own_columns(array, core):
    tokens, width = array.shape
    blocks = array.reshape(tokens, 8, 2, width // 16)
    return lax.dynamic_index_in_dim(blocks, core, 2, keepdims=False).reshape(tokens, width // 2)


def rows_dot(lhs, rhs):
    return lax.dot_general(lhs, rhs, (((0,), (0,)), ((), ())), preferred_element_type=jnp.float32)


def core_summed(lhs, rhs):
    core = lax.axis_index("core")
    sent = rows_dot(own_columns(lhs, 1 - core), rhs).astype(jnp.bfloat16)
    received = passed_along(sent, "core", 1)
    kept = rows_dot(own_columns(lhs, core), rhs)
    return (kept + received.astype(jnp.float32)).astype(jnp.bfloat16)


def wide(array):
    return array.astype(jnp.float32)


def scattered(summed):
    x_at, y_at = (lax.axis_index("x_hi"), lax.axis_index("y"))
    rows = summed.shape[0] // 8
    blocks = summed.reshape(2, 4, rows, summed.shape[1])

    def block(step):
        return lax.dynamic_index_in_dim(blocks, (y_at + step) % 4, 1, keepdims=False)

    far, above, below, mine = (block(2), block(1), block(3), block(0))
    up = from_below(far[0])
    down = from_above(far[1])
    above = jnp.stack([(wide(above[0]) + wide(up)).astype(jnp.bfloat16), above[1]])
    below = jnp.stack([below[0], (wide(below[1]) + wide(down)).astype(jnp.bfloat16)])
    total = wide(mine) + wide(from_below(above)) + wide(from_above(below))
    kept = lax.dynamic_index_in_dim(total, x_at, 0, keepdims=False)
    sent = lax.dynamic_index_in_dim(total, 1 - x_at, 0, keepdims=False).astype(jnp.bfloat16)
    return kept + wide(passed_along(sent, "x_hi", 1))


def rope_tables(length, head_size):
    halfway = head_size // 2
    indices = jnp.arange(halfway, dtype=jnp.float32)
    frequency = rope_base ** (-2.0 * indices / head_size)
    angles = jnp.arange(length, dtype=jnp.float32)[:, None] * frequency[None, :]
    angles = jnp.concatenate([angles, angles], axis=1)
    return (jnp.cos(angles), jnp.sin(angles))


def rotate_half(values):
    halfway = values.shape[-1] // 2
    return jnp.concatenate([-values[..., halfway:], values[..., :halfway]], axis=-1)


def apply_rope(values, cosine_table, sine_table):
    return values * cosine_table[:, None, :] + rotate_half(values) * sine_table[:, None, :]


def unapply_rope(values, cosine_table, sine_table):
    return values * cosine_table[:, None, :] - rotate_half(values * sine_table[:, None, :])


def contract(pattern, first_operand, second_operand):
    return jnp.einsum(pattern, first_operand, second_operand, preferred_element_type=jnp.float32)


def normalize(inputs, gain_values):
    widened = inputs.astype(jnp.float32)
    inv_rms = lax.rsqrt(jnp.mean(widened * widened, axis=-1, keepdims=True) + rms_eps)
    normed = (widened * inv_rms * gain_values).astype(jnp.bfloat16)
    return (widened, inv_rms, normed)


def attention_back(qkv_rows, attn_grad, cosine_table, sine_table):
    tokens_here = qkv_rows.shape[0]
    q_width = HEADS * HEAD_DIM
    kv_width = KV_HEADS * HEAD_DIM
    group_size = HEADS // KV_HEADS
    score_scale = HEAD_DIM ** (-0.5)
    queries = apply_rope(
        qkv_rows[:, :q_width].reshape(tokens_here, HEADS, HEAD_DIM), cosine_table, sine_table
    ).astype(jnp.bfloat16)
    key_heads = apply_rope(
        qkv_rows[:, q_width : q_width + kv_width].reshape(tokens_here, KV_HEADS, HEAD_DIM),
        cosine_table,
        sine_table,
    ).astype(jnp.bfloat16)
    values = (
        qkv_rows[:, q_width + kv_width :]
        .reshape(tokens_here, KV_HEADS, HEAD_DIM)
        .astype(jnp.bfloat16)
    )
    queries = queries.reshape(tokens_here, KV_HEADS, group_size, HEAD_DIM)
    grad_heads = attn_grad.reshape(tokens_here, KV_HEADS, group_size, HEAD_DIM)
    scores = contract("tkgd,ukd->kgtu", queries, key_heads) * score_scale
    row_ids = lax.broadcasted_iota(jnp.int32, (tokens_here, tokens_here), 0)
    col_ids = lax.broadcasted_iota(jnp.int32, (tokens_here, tokens_here), 1)
    causal = col_ids <= row_ids
    exp_scores = jnp.where(causal, jnp.exp(scores), 0.0)
    attention = exp_scores / jnp.sum(exp_scores, axis=-1, keepdims=True)
    attention_low = attention.astype(jnp.bfloat16)
    grad_values = contract("kgtu,tkgd->ukd", attention_low, grad_heads)
    grad_attention = contract("tkgd,ukd->kgtu", grad_heads, values)
    row_delta = jnp.sum(attention * grad_attention, axis=-1, keepdims=True)
    grad_scores = (attention * (grad_attention - row_delta) * score_scale).astype(jnp.bfloat16)
    grad_queries = contract("kgtu,ukd->tkgd", grad_scores, key_heads)
    grad_keys = contract("kgtu,tkgd->ukd", grad_scores, queries)
    grad_queries = unapply_rope(
        grad_queries.reshape(tokens_here, HEADS, HEAD_DIM), cosine_table, sine_table
    )
    grad_keys = unapply_rope(grad_keys, cosine_table, sine_table)
    joined = jnp.concatenate(
        [
            grad_queries.reshape(tokens_here, q_width),
            grad_keys.reshape(tokens_here, kv_width),
            grad_values.reshape(tokens_here, kv_width),
        ],
        axis=1,
    )
    return joined.astype(jnp.bfloat16)


def finish_grad(widened, inv_rms, gain_values, upstream, grad_normed):
    scaled = grad_normed * gain_values
    inner_mean = jnp.mean(scaled * widened, axis=-1, keepdims=True)
    result = upstream.astype(jnp.float32) + inv_rms * scaled - widened * inv_rms**3 * inner_mean
    return result.astype(jnp.bfloat16)


def local(
    layer_inputs, out_grads, attn_stash, proj_grads, w_qkv, w_out, norm_gain, b_sched, w_sched
):
    seq_len = layer_inputs.shape[2]
    cosine_table, sine_table = rope_tables(seq_len, HEAD_DIM)
    gain_values = norm_gain[0]
    b_slot = b_sched[0]
    w_slot = w_sched[0]
    contract_cols = (((1,), (1,)), ((), ()))
    whole_qkv = assembled(w_qkv[0])
    whole_out = assembled(w_out[0])
    inputs_w = lax.dynamic_index_in_dim(layer_inputs[0], w_slot, 0, keepdims=False)
    upstream_w = lax.dynamic_index_in_dim(out_grads[0], w_slot, 0, keepdims=False)
    attended_w = lax.dynamic_index_in_dim(attn_stash[0], w_slot, 0, keepdims=False)
    projected_w = lax.dynamic_index_in_dim(proj_grads[0], w_slot, 0, keepdims=False)
    unused_wide, unused_inv, normed_w = normalize(inputs_w, gain_values)
    summed_qkv = core_summed(normed_w, projected_w)
    summed_out = core_summed(attended_w, upstream_w)
    inputs_b = lax.dynamic_index_in_dim(layer_inputs[0], b_slot, 0, keepdims=False)
    upstream_b = lax.dynamic_index_in_dim(out_grads[0], b_slot, 0, keepdims=False)
    widened, inv_rms, normed = normalize(inputs_b, gain_values)
    whole_qkv, whole_out, summed_qkv, summed_out = lax.optimization_barrier(
        (whole_qkv, whole_out, summed_qkv, summed_out)
    )
    grad_qkv_w = scattered(summed_qkv)
    grad_out_w = scattered(summed_out)
    qkv_rows = jnp.dot(normed, whole_qkv, preferred_element_type=jnp.float32)
    attn_grad = lax.dot_general(
        upstream_b, whole_out, contract_cols, preferred_element_type=jnp.float32
    ).astype(jnp.bfloat16)
    grad_proj = attention_back(qkv_rows, attn_grad, cosine_table, sine_table)
    grad_normed = lax.dot_general(
        grad_proj, whole_qkv, contract_cols, preferred_element_type=jnp.float32
    )
    sent_grads = finish_grad(widened, inv_rms, gain_values, upstream_b, grad_normed)
    sent_back = passed_along(sent_grads, SECTION, -1)[None]
    return (sent_back, grad_qkv_w[None], grad_out_w[None])


def solution(mesh):
    finer = Mesh(
        mesh.devices.reshape(mesh.shape["section"] // 2, 2, 2, 4, 2), SECTION + FSDP
    )
    return jax.shard_map(
        local,
        mesh=finer,
        in_specs=(
            P(SECTION, None, FSDP, None),
            P(SECTION, None, FSDP, None),
            P(SECTION, None, FSDP, None),
            P(SECTION, None, FSDP, None),
            P(SECTION, FSDP, None),
            P(SECTION, FSDP, None),
            P(SECTION, None),
            P(SECTION),
            P(SECTION),
        ),
        out_specs=(P(SECTION, FSDP, None), P(SECTION, FSDP, None), P(SECTION, FSDP, None)),
        check_vma=False,
    )
```

```python
import jax
import jax.numpy as jnp
from jax import lax
from jax.experimental import pallas as pl
from jax.experimental.pallas import tpu as pltpu
from jax.sharding import Mesh
from jax.sharding import PartitionSpec as P


HEAD_DIM = 64
KV_HEADS = 4
SECTION = ("z", "x_lo")
FSDP = ("x_hi", "y", "core")
SEQ = 384
D = 2048
QW = 1024
WIDTH = 1536
BLOCK = 512
Q_ROWS = 384
PIECE = 640
TILE = 128


rms_eps = 1e-05
rope_base = 500000.0
f32 = jnp.float32
bf16 = jnp.bfloat16

GROUPS = (((0, 0), (1, 0)), ((0, 1), (0, 3)), ((1, 1), (1, 3)), ((0, 2), (1, 2)))

VMEM = pl.BlockSpec(memory_space=pltpu.VMEM)
SMEM = pl.BlockSpec(memory_space=pltpu.SMEM)
HBM = pl.BlockSpec(memory_space=pltpu.HBM)


def passed_along(array, axis, by):
    size = lax.axis_size(axis)
    return lax.ppermute(array, axis, [(i, (i + by) % size) for i in range(size)])


def from_above(array):
    return passed_along(array, "y", -1)


def from_below(array):
    return passed_along(array, "y", 1)


def limit(mebibytes):
    return pltpu.CompilerParams(vmem_limit_bytes=mebibytes << 20)


def pack_body(qkv, out, packed):
    for j in range(3):
        packed[j * TILE : (j + 1) * TILE, :] = qkv[0, :, j * BLOCK : (j + 1) * BLOCK]
    for j in range(4):
        packed[Q_ROWS + j * HEAD_DIM : Q_ROWS + (j + 1) * HEAD_DIM, :] = out[
            0, :, j * BLOCK : (j + 1) * BLOCK
        ]


def packed_shard(qkv, out):
    return pl.pallas_call(
        pack_body,
        in_specs=[VMEM, VMEM],
        out_specs=VMEM,
        out_shape=jax.ShapeDtypeStruct((PIECE, BLOCK), bf16),
        compiler_params=limit(4),
        name="pack",
    )(qkv, out)


def gathered_groups(shard):
    other = passed_along(shard, "x_hi", 1)
    above, below = (from_above(shard), from_below(shard))
    above_other = from_above(other)
    below_other = from_below(other)
    far = from_above(above)
    far_other = from_below(below_other)

    def with_peer(array):
        return (array, passed_along(array, "core", 1))

    return (
        (*with_peer(shard), *with_peer(other)),
        (*with_peer(above), *with_peer(below)),
        (*with_peer(above_other), *with_peer(below_other)),
        (*with_peer(far), *with_peer(far_other)),
    )


def rope_tables(length):
    halfway = HEAD_DIM // 2
    indices = jnp.arange(halfway, dtype=f32)
    frequency = rope_base ** (-2.0 * indices / HEAD_DIM)
    angles = jnp.arange(length, dtype=f32)[:, None] * frequency[None, :]
    angles = jnp.concatenate([angles] * 4, axis=1)
    return (jnp.cos(angles), jnp.sin(angles))


def nt(lhs, rhs):
    return lax.dot_general(lhs, rhs, (((1,), (1,)), ((), ())), preferred_element_type=f32)


def tn(lhs, rhs):
    return lax.dot_general(lhs, rhs, (((0,), (0,)), ((), ())), preferred_element_type=f32)


def nn(lhs, rhs):
    return jnp.dot(lhs, rhs, preferred_element_type=f32)


def chip_of(at, dx, dy):
    x_at = at[0] if dx == 0 else 1 - at[0]
    return x_at * 4 + lax.rem(at[1] + dy, 4)


def qkv_block(piece, j):
    return piece[j * TILE : (j + 1) * TILE, :]


def out_block(piece, j):
    return piece[Q_ROWS + j * HEAD_DIM : Q_ROWS + (j + 1) * HEAD_DIM, :]


def inverse_rms(rows):
    return lax.rsqrt(jnp.mean(rows * rows, axis=-1, keepdims=True) + rms_eps)


def chips_of(at, keys):
    return [chip_of(at, dx, dy) for pair in keys for dx, dy in pair]


def relative_columns(at, normed, keys, rel):
    core = at[2]
    for n, chip in enumerate(chips_of(at, keys)):
        for half, place in ((0, core), (1, 1 - core)):
            cols = pl.ds(pl.multiple_of((chip * 2 + place) * TILE, TILE), TILE)
            rel[:, (2 * n + half) * TILE : (2 * n + half + 1) * TILE] = normed[:, cols]


def project_rows(rel, pieces, acc_init, acc):
    for j in range(3):
        rows = [qkv_block(piece, j) for piece in pieces]
        cols = slice(j * BLOCK, (j + 1) * BLOCK)
        total = nn(rel, jnp.concatenate(rows, axis=0))
        if acc_init is not None:
            total = total + acc_init[:, cols]
        acc[:, cols] = total


def project_heads(at, upstream, pieces, keys, attn_grad):
    core = at[2]
    heads = None
    for j in range(4):
        rows = [out_block(piece, j) for piece in pieces]
        part = nt(upstream[:, j * BLOCK : (j + 1) * BLOCK], jnp.concatenate(rows, axis=0))
        heads = part if heads is None else heads + part
    for n, chip in enumerate(chips_of(at, keys)):
        block = heads[:, n * TILE : (n + 1) * TILE]
        block = jnp.where(core == 0, block, pltpu.roll(block, HEAD_DIM, 1))
        attn_grad[:, pl.ds(pl.multiple_of(chip * TILE, TILE), TILE)] = block.astype(bf16)


def first_body(
    at, x_all, g_all, gain, *refs
):
    pieces, (acc, attn_grad, rest, x, g, normed, rel, sems) = (refs[:8], refs[8:])
    copies = [
        pltpu.make_async_copy(x_all.at[0, at[3]], x, sems.at[0]),
        pltpu.make_async_copy(g_all.at[0, at[3]], g, sems.at[1]),
    ]
    for copy in copies:
        copy.start()
    copies[0].wait()

    def norm_rows(i, carry):
        rows = pl.ds(pl.multiple_of(i * 32, 32), 32)
        wide = x[rows, :].astype(f32)
        normed[rows, :] = (wide * inverse_rms(wide) * gain[...]).astype(bf16)
        return carry

    lax.fori_loop(0, SEQ // 32, norm_rows, 0)
    relative_columns(at, normed, GROUPS[:2], rel)
    relative_columns(at, normed, GROUPS[2:], rest)
    project_rows(rel[...], pieces, None, acc)
    copies[1].wait()
    project_heads(at, g, pieces, GROUPS[:2], attn_grad)


def first_stage(at, layer_inputs, out_grads, gain, groups):
    pieces = [array for pair in groups for array in pair]
    return pl.pallas_call(
        first_body,
        in_specs=[SMEM, HBM, HBM] + [VMEM] * (1 + 8),
        out_specs=[VMEM] * 3,
        out_shape=[
            jax.ShapeDtypeStruct((SEQ, WIDTH), f32),
            jax.ShapeDtypeStruct((SEQ, QW), bf16),
            jax.ShapeDtypeStruct((SEQ, QW), bf16),
        ],
        scratch_shapes=[
            pltpu.VMEM((SEQ, D), bf16),
            pltpu.VMEM((SEQ, D), bf16),
            pltpu.VMEM((SEQ, D), bf16),
            pltpu.VMEM((SEQ, QW), bf16),
            pltpu.SemaphoreType.DMA((2,)),
        ],
        compiler_params=limit(24),
        name="first_stage",
    )(at, layer_inputs, out_grads, gain, *pieces)


def more_body(at, g_all, acc_in, attn_in, rest, *refs):
    pieces, (acc, attn_grad, g, sems) = (refs[:4], refs[4:])
    copy = pltpu.make_async_copy(g_all.at[0, at[3]], g, sems.at[0])
    copy.start()
    attn_grad[...] = attn_in[...]
    project_rows(rest[:, : 4 * TILE], pieces, acc_in, acc)
    copy.wait()
    project_heads(at, g, pieces, GROUPS[2:3], attn_grad)


def more_stage(at, out_grads, acc, attn_grad, rest, group):
    return pl.pallas_call(
        more_body,
        in_specs=[SMEM, HBM] + [VMEM] * 7,
        out_specs=[VMEM] * 2,
        out_shape=[jax.ShapeDtypeStruct((SEQ, WIDTH), f32), jax.ShapeDtypeStruct((SEQ, QW), bf16)],
        scratch_shapes=[pltpu.VMEM((SEQ, D), bf16), pltpu.SemaphoreType.DMA((1,))],
        compiler_params=limit(20),
        name="more_stage",
    )(at, out_grads, acc, attn_grad, rest, *group)


def whole_spec(shape):
    return pl.BlockSpec(shape, lambda i, at: (0,) * len(shape))


def first_half_lanes(rows):
    lanes = lax.broadcasted_iota(jnp.int32, (rows, TILE), 1)
    return lax.rem(lanes, HEAD_DIM) < HEAD_DIM // 2


def rope(u, cosine, sine):
    turned = jnp.where(
        first_half_lanes(u.shape[0]), -pltpu.roll(u, TILE - 32, 1), pltpu.roll(u, 32, 1)
    )
    return u * cosine + turned * sine


def unrope(u, cosine, sine):
    v = u * sine
    turned = jnp.where(
        first_half_lanes(u.shape[0]), -pltpu.roll(v, TILE - 32, 1), pltpu.roll(v, 32, 1)
    )
    return u * cosine - turned


def lower_lanes(rows):
    return lax.broadcasted_iota(jnp.int32, (rows, TILE), 1) < HEAD_DIM


def key_half(block, group):
    wide = block.astype(f32)
    if group % 2:
        wide = pltpu.roll(wide, HEAD_DIM, 1)
    return jnp.where(lower_lanes(block.shape[0]), wide, 0.0)


def stacked_heads(source, tile_rows, group):
    parts = []
    for pair in range(2):
        block = source[tile_rows, (2 * group + pair) * TILE : (2 * group + pair + 1) * TILE]
        parts += [block, pltpu.roll(block.astype(f32), HEAD_DIM, 1).astype(bf16)]
    return jnp.concatenate(parts, axis=0)


def attention_tile(qkv, attn_grad, tile, group, grad_q, grad_k, grad_v, fresh):
    count = (tile + 1) * TILE
    tile_rows = slice(tile * TILE, count)
    at_key = QW + (group // 2) * TILE
    at_value = at_key + 2 * TILE
    keys = (key_half(qkv[:count, at_key : at_key + TILE], group) * 0.125).astype(bf16)
    values = key_half(qkv[:count, at_value : at_value + TILE], group).astype(bf16)
    queries = stacked_heads(qkv, tile_rows, group)
    grads = stacked_heads(attn_grad, tile_rows, group)
    weights = jnp.exp(nt(keys, queries))
    key_ids = lax.broadcasted_iota(jnp.int32, (TILE, 4 * TILE), 0)
    query_ids = lax.rem(lax.broadcasted_iota(jnp.int32, (TILE, 4 * TILE), 1), TILE)
    last = jnp.where(key_ids <= query_ids, weights[tile * TILE :], 0.0)
    weights = last if tile == 0 else jnp.concatenate([weights[: tile * TILE], last], axis=0)
    probs = weights * (1.0 / jnp.sum(weights, axis=0, keepdims=True))
    grad_probs = nt(values, grads)
    delta = jnp.sum(probs * grad_probs, axis=0, keepdims=True)
    grad_scores = (probs * (grad_probs - delta)).astype(bf16)
    value_part = nn(probs.astype(bf16), grads)
    key_part = nn(grad_scores, queries) * 0.125
    if fresh:
        grad_v[group, :count, :] = value_part
        grad_k[group, :count, :] = key_part
    else:
        grad_v[group, :count, :] += value_part
        grad_k[group, :count, :] += key_part
    turned = tn(keys, grad_scores)[:HEAD_DIM]
    for pair in range(2):
        both = jnp.concatenate(
            [turned[:, (2 * pair + i) * TILE : (2 * pair + i + 1) * TILE] for i in range(2)], axis=0
        )
        grad_q(2 * group + pair, both.T)


def finish_rows(at, rows, grad_proj, pieces, x, g, gain, grad_normed, out):
    core = at[2]
    for n, chip in enumerate(chips_of(at, GROUPS)):
        both = jnp.concatenate(
            [
                jnp.concatenate([qkv_block(piece, j) for j in range(3)], axis=1)
                for piece in pieces[2 * n : 2 * n + 2]
            ],
            axis=0,
        )
        part = nt(grad_proj[...], both)
        for half, place in ((0, core), (1, 1 - core)):
            cols = pl.ds(pl.multiple_of((chip * 2 + place) * TILE, TILE), TILE)
            grad_normed[:, cols] = part[:, half * TILE : (half + 1) * TILE]

    def norm_rows(i, carry):
        here = pl.ds(pl.multiple_of(i * 16, 16), 16)
        wide = x[here, :].astype(f32)
        inv = inverse_rms(wide)
        scaled = grad_normed[here, :] * gain[...]
        inner = jnp.mean(scaled * wide, axis=-1, keepdims=True)
        result = g[here, :].astype(f32) + inv * scaled - wide * (inv * inv * inv * inner)
        out[here, :] = result.astype(bf16)
        return carry

    lax.fori_loop(0, rows // 16, norm_rows, 0)


def join_keys(grad_k, grad_v, rows, cosine, sine, grad_proj):
    lower = lower_lanes(TILE)
    for pair in range(2):
        for first in range(rows[0], rows[1], TILE):
            here = slice(first, first + TILE)
            there = slice(first - rows[0], first - rows[0] + TILE)
            k = jnp.where(
                lower,
                grad_k[2 * pair, here, :],
                pltpu.roll(grad_k[2 * pair + 1, here, :], HEAD_DIM, 1),
            )
            v = jnp.where(
                lower,
                grad_v[2 * pair, here, :],
                pltpu.roll(grad_v[2 * pair + 1, here, :], HEAD_DIM, 1),
            )
            at_key = QW + pair * TILE
            grad_proj[there, at_key : at_key + TILE] = unrope(
                k, cosine[here, :], sine[here, :]
            ).astype(bf16)
            grad_proj[there, at_key + 2 * TILE : at_key + 3 * TILE] = v.astype(bf16)


def store_query_grads(grad_proj, there, cosine, sine):
    def store(block, value):
        grad_proj[there, block * TILE : (block + 1) * TILE] = unrope(value, cosine, sine).astype(bf16)

    return store


def second_body(
    at, x_all, g_all, gain, cosine, sine, acc_in, attn_in, rest, *refs
):
    pieces, (out, qkv_first, attn_first, grad_k_first, grad_v_first) = (refs[:16], refs[16:21])
    x, g, acc, attn_grad, qkv, grad_k, grad_v, grad_proj, grad_normed, sems = refs[21:]
    slot = at[3]
    copies = [
        pltpu.make_async_copy(g_all.at[0, slot], g, sems.at[1]),
        pltpu.make_async_copy(x_all.at[0, slot, pl.ds(TILE, 2 * TILE)], x, sems.at[0]),
    ]
    for copy in copies:
        copy.start()
    attn_grad[...] = attn_in[...]
    project_rows(rest[:, 4 * TILE :], pieces[12:], acc_in, acc)
    for block in range(10):
        cols = slice(block * TILE, (block + 1) * TILE)
        qkv[:, cols] = rope(acc[:, cols], cosine[...], sine[...]).astype(bf16)
    qkv[:, 10 * TILE :] = acc[:, 10 * TILE :].astype(bf16)
    copies[0].wait()
    project_heads(at, g, pieces[12:], GROUPS[3:], attn_grad)
    for group in range(KV_HEADS):
        for tile in (2, 1):
            here = slice(tile * TILE, (tile + 1) * TILE)
            there = slice((tile - 1) * TILE, tile * TILE)
            store = store_query_grads(grad_proj, there, cosine[here, :], sine[here, :])
            attention_tile(qkv, attn_grad, tile, group, store, grad_k, grad_v, tile == 2)
    join_keys(grad_k, grad_v, (TILE, SEQ), cosine, sine, grad_proj)
    copies[1].wait()
    finish_rows(at, 2 * TILE, grad_proj, pieces, x, g.at[TILE:], gain, grad_normed, out)
    qkv_first[...] = qkv[:TILE, :]
    attn_first[...] = attn_grad[:TILE, :]
    grad_k_first[...] = grad_k[:, :TILE, :]
    grad_v_first[...] = grad_v[:, :TILE, :]


def second_stage(at, layer_inputs, out_grads, gain, tables, acc, attn_grad, rest, groups):
    pieces = [array for pair in groups for array in pair]
    return pl.pallas_call(
        second_body,
        in_specs=[SMEM, HBM, HBM] + [VMEM] * (6 + 16),
        out_specs=[VMEM] * 5,
        out_shape=[
            jax.ShapeDtypeStruct((2 * TILE, D), bf16),
            jax.ShapeDtypeStruct((TILE, WIDTH), bf16),
            jax.ShapeDtypeStruct((TILE, QW), bf16),
            jax.ShapeDtypeStruct((KV_HEADS, TILE, TILE), f32),
            jax.ShapeDtypeStruct((KV_HEADS, TILE, TILE), f32),
        ],
        scratch_shapes=[
            pltpu.VMEM((2 * TILE, D), bf16),
            pltpu.VMEM((SEQ, D), bf16),
            pltpu.VMEM((SEQ, WIDTH), f32),
            pltpu.VMEM((SEQ, QW), bf16),
            pltpu.VMEM((SEQ, WIDTH), bf16),
            pltpu.VMEM((KV_HEADS, SEQ, TILE), f32),
            pltpu.VMEM((KV_HEADS, SEQ, TILE), f32),
            pltpu.VMEM((2 * TILE, WIDTH), bf16),
            pltpu.VMEM((2 * TILE, D), f32),
            pltpu.SemaphoreType.DMA((2,)),
        ],
        compiler_params=limit(24),
        name="second_stage",
    )(at, layer_inputs, out_grads, gain, *tables, acc, attn_grad, rest, *pieces)


def third_body(
    at, x_all, g_all, gain, cosine, sine, qkv, attn_grad, grad_k_in, grad_v_in, *refs
):
    pieces, (out, x, g, grad_k, grad_v, grad_proj, grad_normed, sems) = (refs[:16], refs[16:])
    slot = at[3]
    copies = [
        pltpu.make_async_copy(x_all.at[0, slot, pl.ds(0, TILE)], x, sems.at[0]),
        pltpu.make_async_copy(g_all.at[0, slot, pl.ds(0, TILE)], g, sems.at[1]),
    ]
    for copy in copies:
        copy.start()
    grad_k[...] = grad_k_in[...]
    grad_v[...] = grad_v_in[...]
    here = slice(0, TILE)
    store = store_query_grads(grad_proj, here, cosine[here, :], sine[here, :])
    for group in range(KV_HEADS):
        attention_tile(qkv, attn_grad, 0, group, store, grad_k, grad_v, False)
    join_keys(grad_k, grad_v, (0, TILE), cosine, sine, grad_proj)
    for copy in copies:
        copy.wait()
    finish_rows(at, TILE, grad_proj, pieces, x, g, gain, grad_normed, out)


def third_stage(at, layer_inputs, out_grads, gain, tables, carried, groups):
    pieces = [array for pair in groups for array in pair]
    return pl.pallas_call(
        third_body,
        in_specs=[SMEM, HBM, HBM] + [VMEM] * (7 + 16),
        out_specs=VMEM,
        out_shape=jax.ShapeDtypeStruct((TILE, D), bf16),
        scratch_shapes=[
            pltpu.VMEM((TILE, D), bf16),
            pltpu.VMEM((TILE, D), bf16),
            pltpu.VMEM((KV_HEADS, TILE, TILE), f32),
            pltpu.VMEM((KV_HEADS, TILE, TILE), f32),
            pltpu.VMEM((TILE, WIDTH), bf16),
            pltpu.VMEM((TILE, D), f32),
            pltpu.SemaphoreType.DMA((2,)),
        ],
        compiler_params=limit(24),
        name="third_stage",
    )(at, layer_inputs, out_grads, gain, *tables, *carried, *pieces)


def weight_body(at, x_all, p_all, a_all, e_all, gain, sent, kept, x, p, a, e, inv, sems):
    step = pl.program_id(0)
    slot = at[3]
    copies = [
        pltpu.make_async_copy(whole.at[0, slot], part, sems.at[n])
        for n, (whole, part) in enumerate(((x_all, x), (p_all, p), (a_all, a), (e_all, e)))
    ]

    @pl.when(step == 0)
    def _():
        for copy in copies:
            copy.start()
        copies[0].wait()

        def norm_rows(i, carry):
            rows = pl.ds(pl.multiple_of(i * 32, 32), 32)
            inv[rows, :] = jnp.broadcast_to(inverse_rms(x[rows, :].astype(f32)), (32, TILE))
            return carry

        lax.fori_loop(0, SEQ // 32, norm_rows, 0)
        for copy in copies[1:]:
            copy.wait()

    flip = lax.rem(step, 2)
    x_at = at[0] + flip - 2 * at[0] * flip
    chip = x_at * 4 + lax.rem(at[1] + step // 2, 4)
    cols = pl.ds(pl.multiple_of(chip * 2 * TILE, 2 * TILE), 2 * TILE)
    scale = jnp.concatenate([inv[...], inv[...]], axis=1)
    normed = (x[:, cols].astype(f32) * scale * gain[:, cols]).astype(bf16)
    part = tn(normed, p[...])
    core_zero = at[2] == 0
    for j in range(3):
        where = slice(j * TILE, (j + 1) * TILE)
        top = part[:TILE, j * BLOCK : (j + 1) * BLOCK].astype(bf16)
        low = part[TILE:, j * BLOCK : (j + 1) * BLOCK].astype(bf16)
        kept[0, where, :] = jnp.where(core_zero, top, low)
        sent[0, where, :] = jnp.where(core_zero, low, top)
    heads = a[:, pl.ds(pl.multiple_of(chip * TILE, TILE), TILE)]
    part = tn(heads, e[...])
    for j in range(4):
        where = slice(Q_ROWS + j * HEAD_DIM, Q_ROWS + (j + 1) * HEAD_DIM)
        top = part[:HEAD_DIM, j * BLOCK : (j + 1) * BLOCK].astype(bf16)
        low = part[HEAD_DIM:, j * BLOCK : (j + 1) * BLOCK].astype(bf16)
        kept[0, where, :] = jnp.where(core_zero, top, low)
        sent[0, where, :] = jnp.where(core_zero, low, top)


def weight_stage(at, layer_inputs, proj_grads, attn_stash, out_grads, gain):
    block = pl.BlockSpec((1, PIECE, BLOCK), lambda i, at: (lax.rem(i, 2) * 4 + i // 2, 0, 0))
    shape = jax.ShapeDtypeStruct((8, PIECE, BLOCK), bf16)
    return pl.pallas_call(
        weight_body,
        grid_spec=pltpu.PrefetchScalarGridSpec(
            num_scalar_prefetch=1,
            grid=(8,),
            in_specs=[HBM] * 4 + [whole_spec((1, D))],
            out_specs=[block, block],
            scratch_shapes=[
                pltpu.VMEM((SEQ, D), bf16),
                pltpu.VMEM((SEQ, WIDTH), bf16),
                pltpu.VMEM((SEQ, QW), bf16),
                pltpu.VMEM((SEQ, D), bf16),
                pltpu.VMEM((SEQ, TILE), f32),
                pltpu.SemaphoreType.DMA((4,)),
            ],
        ),
        out_shape=[shape, shape],
        compiler_params=limit(56),
        name="weight_stage",
    )(at, layer_inputs, proj_grads, attn_stash, out_grads, gain)


def wide(array):
    return array.astype(f32)


def prepare_body(kept, received, up, down, k, r, sems):
    copies = []
    for n in range(2):
        far = (4 * n + 2, pl.ds(0, Q_ROWS))
        copies.append(pltpu.make_async_copy(kept.at[far], k.at[n], sems.at[2 * n]))
        copies.append(pltpu.make_async_copy(received.at[far], r.at[n], sems.at[2 * n + 1]))
    for copy in copies:
        copy.start()
    for copy in copies:
        copy.wait()
    for n, out in enumerate((up, down)):
        out[...] = (wide(k[n]) + wide(r[n])).astype(bf16)


def prepare_stage(kept, received):
    shape = jax.ShapeDtypeStruct((Q_ROWS, BLOCK), bf16)
    return pl.pallas_call(
        prepare_body,
        in_specs=[HBM] * 2,
        out_specs=[VMEM] * 2,
        out_shape=[shape, shape],
        scratch_shapes=[
            pltpu.VMEM((2, Q_ROWS, BLOCK), bf16),
            pltpu.VMEM((2, Q_ROWS, BLOCK), bf16),
            pltpu.SemaphoreType.DMA((4,)),
        ],
        compiler_params=limit(10),
        name="prepare",
    )(kept, received)


def final_body(mine, last, qkv):
    total = mine[...] + last[...].astype(f32)
    for j in range(3):
        qkv[0, :, j * BLOCK : (j + 1) * BLOCK] = total[j * TILE : (j + 1) * TILE]


def final_sum(mine, last):
    return pl.pallas_call(
        final_body,
        in_specs=[VMEM] * 2,
        out_specs=VMEM,
        out_shape=jax.ShapeDtypeStruct((1, TILE, WIDTH), f32),
        compiler_params=limit(6),
        name="final_sum",
    )(mine, last)


def scattered(sent, kept):
    received = passed_along(sent, "core", 1)
    across = (wide(kept[4:, Q_ROWS:]) + wide(received[4:, Q_ROWS:])).astype(bf16)
    across = passed_along(across, "x_hi", 1)
    up, down = prepare_stage(kept, received)
    up = wide(from_below(up))
    down = wide(from_above(down))
    half = (PIECE - Q_ROWS) // 2

    def qkv_sum(dx, dy):
        at = 4 * dx + dy
        return wide(kept[at, :Q_ROWS]) + wide(received[at, :Q_ROWS])

    def out_sum(dy):
        return wide(kept[dy, Q_ROWS:]) + wide(received[dy, Q_ROWS:]) + wide(across[dy])

    above = jnp.concatenate([qkv_sum(0, 1) + up, qkv_sum(1, 1)])
    below = jnp.concatenate([qkv_sum(0, 3), qkv_sum(1, 3) + down])
    above = wide(from_below(above.astype(bf16)))
    below = wide(from_above(below.astype(bf16)))
    far, out_above, out_below = (out_sum(2).astype(bf16), out_sum(1), out_sum(3))
    up = wide(from_below(far[:half]))
    down = wide(from_above(far[half:]))
    out_above = jnp.concatenate([out_above[:half] + up, out_above[half:]])
    out_below = jnp.concatenate([out_below[:half], out_below[half:] + down])
    out_above = wide(from_below(out_above.astype(bf16)))
    out_below = wide(from_above(out_below.astype(bf16)))
    kept_rows = qkv_sum(0, 0) + above[:Q_ROWS] + below[:Q_ROWS]
    sent_rows = qkv_sum(1, 0) + above[Q_ROWS:] + below[Q_ROWS:]
    last = passed_along(sent_rows.astype(bf16), "x_hi", 1)
    out = out_sum(0) + out_above + out_below
    out = jnp.concatenate([out[j * HEAD_DIM : (j + 1) * HEAD_DIM] for j in range(4)], axis=1)
    return (final_sum(kept_rows, last), out[None])


def local_step(
    layer_inputs, out_grads, attn_stash, proj_grads, w_qkv, w_out, norm_gain, b_sched, w_sched
):
    tables = rope_tables(SEQ)
    place = [lax.axis_index(name) for name in FSDP]
    at_b = jnp.stack([*place, b_sched[0]]).astype(jnp.int32)
    at_w = jnp.stack([*place, w_sched[0]]).astype(jnp.int32)
    groups = gathered_groups(packed_shard(w_qkv, w_out))
    sent, kept = weight_stage(at_w, layer_inputs, proj_grads, attn_stash, out_grads, norm_gain)
    acc, attn_grad, rest = first_stage(at_b, layer_inputs, out_grads, norm_gain, groups[:2])
    acc, attn_grad = more_stage(at_b, out_grads, acc, attn_grad, rest, groups[2])
    grads = scattered(sent, kept)
    second, *carried = second_stage(
        at_b, layer_inputs, out_grads, norm_gain, tables, acc, attn_grad, rest, groups
    )
    second = passed_along(second, SECTION, -1)
    first = third_stage(at_b, layer_inputs, out_grads, norm_gain, tables, carried, groups)
    first = passed_along(first, SECTION, -1)
    sent_back = jnp.concatenate([first, second], axis=0)
    return (sent_back[None], *grads)


def solution(mesh):
    finer = Mesh(mesh.devices.reshape(mesh.shape["section"] // 2, 2, 2, 4, 2), SECTION + FSDP)
    return jax.shard_map(
        local_step,
        mesh=finer,
        in_specs=(
            P(SECTION, None, FSDP, None),
            P(SECTION, None, FSDP, None),
            P(SECTION, None, FSDP, None),
            P(SECTION, None, FSDP, None),
            P(SECTION, FSDP, None),
            P(SECTION, FSDP, None),
            P(SECTION, None),
            P(SECTION),
            P(SECTION),
        ),
        out_specs=(P(SECTION, FSDP, None), P(SECTION, FSDP, None), P(SECTION, FSDP, None)),
        check_vma=False,
    )
```

```python
import jax
import jax.numpy as jnp
from jax import lax
from jax.experimental import pallas as pl
from jax.experimental.pallas import tpu as pltpu
from jax.sharding import Mesh
from jax.sharding import PartitionSpec as P


HEAD_DIM = 64
KV_HEADS = 4
SECTION = ("z", "x_lo")
FSDP = ("x_hi", "y", "core")
SEQ = 384
D = 2048
QW = 1024
WIDTH = 1536
BLOCK = 512
Q_ROWS = 384
PIECE = 640
TILE = 128


rms_eps = 1e-05
rope_base = 500000.0
f32 = jnp.float32
bf16 = jnp.bfloat16

GROUPS = (((0, 0), (1, 0)), ((0, 1), (0, 3)), ((1, 1), (1, 3)), ((0, 2), (1, 2)))

VMEM = pl.BlockSpec(memory_space=pltpu.VMEM)
SMEM = pl.BlockSpec(memory_space=pltpu.SMEM)
HBM = pl.BlockSpec(memory_space=pltpu.HBM)


def passed_along(array, axis, by):
    size = lax.axis_size(axis)
    return lax.ppermute(array, axis, [(i, (i + by) % size) for i in range(size)])


def from_above(array):
    return passed_along(array, "y", -1)


def from_below(array):
    return passed_along(array, "y", 1)


def limit(mebibytes):
    return pltpu.CompilerParams(vmem_limit_bytes=mebibytes << 20)


def pack_body(qkv, out, packed):
    for j in range(3):
        packed[j * TILE : (j + 1) * TILE, :] = qkv[0, :, j * BLOCK : (j + 1) * BLOCK]
    for j in range(4):
        packed[Q_ROWS + j * HEAD_DIM : Q_ROWS + (j + 1) * HEAD_DIM, :] = out[
            0, :, j * BLOCK : (j + 1) * BLOCK
        ]


def packed_shard(qkv, out):
    return pl.pallas_call(
        pack_body,
        in_specs=[VMEM, VMEM],
        out_specs=VMEM,
        out_shape=jax.ShapeDtypeStruct((PIECE, BLOCK), bf16),
        compiler_params=limit(4),
        name="pack",
    )(qkv, out)


def gathered_groups(shard):
    other = passed_along(shard, "x_hi", 1)
    above, below = (from_above(shard), from_below(shard))
    above_other = from_above(other)
    below_other = from_below(other)
    far = from_above(above)
    far_other = from_below(below_other)

    def with_peer(array):
        return (array, passed_along(array, "core", 1))

    return (
        (*with_peer(shard), *with_peer(other)),
        (*with_peer(above), *with_peer(below)),
        (*with_peer(above_other), *with_peer(below_other)),
        (*with_peer(far), *with_peer(far_other)),
    )


def rope_tables(length):
    halfway = HEAD_DIM // 2
    indices = jnp.arange(halfway, dtype=f32)
    frequency = rope_base ** (-2.0 * indices / HEAD_DIM)
    angles = jnp.arange(length, dtype=f32)[:, None] * frequency[None, :]
    angles = jnp.concatenate([angles] * 4, axis=1)
    return (jnp.cos(angles), jnp.sin(angles))


def nt(lhs, rhs):
    return lax.dot_general(lhs, rhs, (((1,), (1,)), ((), ())), preferred_element_type=f32)


def tn(lhs, rhs):
    return lax.dot_general(lhs, rhs, (((0,), (0,)), ((), ())), preferred_element_type=f32)


def nn(lhs, rhs):
    return jnp.dot(lhs, rhs, preferred_element_type=f32)


def chip_of(at, dx, dy):
    x_at = at[0] if dx == 0 else 1 - at[0]
    return x_at * 4 + lax.rem(at[1] + dy, 4)


def qkv_block(piece, j):
    return piece[j * TILE : (j + 1) * TILE, :]


def out_block(piece, j):
    return piece[Q_ROWS + j * HEAD_DIM : Q_ROWS + (j + 1) * HEAD_DIM, :]


def inverse_rms(rows):
    return lax.rsqrt(jnp.mean(rows * rows, axis=-1, keepdims=True) + rms_eps)


def chips_of(at, keys):
    return [chip_of(at, dx, dy) for pair in keys for dx, dy in pair]


def relative_columns(at, normed, keys, rel):
    core = at[2]
    for n, chip in enumerate(chips_of(at, keys)):
        for half, place in ((0, core), (1, 1 - core)):
            cols = pl.ds(pl.multiple_of((chip * 2 + place) * TILE, TILE), TILE)
            rel[:, (2 * n + half) * TILE : (2 * n + half + 1) * TILE] = normed[:, cols]


def project_rows(rel, pieces, acc_init, acc):
    for j in range(3):
        rows = [qkv_block(piece, j) for piece in pieces]
        cols = slice(j * BLOCK, (j + 1) * BLOCK)
        total = nn(rel, jnp.concatenate(rows, axis=0))
        if acc_init is not None:
            total = total + acc_init[:, cols]
        acc[:, cols] = total


def project_heads(at, upstream, pieces, keys, attn_grad):
    core = at[2]
    heads = None
    for j in range(4):
        rows = [out_block(piece, j) for piece in pieces]
        part = nt(upstream[:, j * BLOCK : (j + 1) * BLOCK], jnp.concatenate(rows, axis=0))
        heads = part if heads is None else heads + part
    for n, chip in enumerate(chips_of(at, keys)):
        block = heads[:, n * TILE : (n + 1) * TILE]
        block = jnp.where(core == 0, block, pltpu.roll(block, HEAD_DIM, 1))
        attn_grad[:, pl.ds(pl.multiple_of(chip * TILE, TILE), TILE)] = block.astype(bf16)


def first_body(
    at, x_all, g_all, gain, *refs
):
    pieces, (acc, attn_grad, rest, x, g, normed, rel, sems) = (refs[:8], refs[8:])
    copies = [
        pltpu.make_async_copy(x_all.at[0, at[3]], x, sems.at[0]),
        pltpu.make_async_copy(g_all.at[0, at[3]], g, sems.at[1]),
    ]
    for copy in copies:
        copy.start()
    copies[0].wait()

    def norm_rows(i, carry):
        rows = pl.ds(pl.multiple_of(i * 32, 32), 32)
        wide = x[rows, :].astype(f32)
        normed[rows, :] = (wide * inverse_rms(wide) * gain[...]).astype(bf16)
        return carry

    lax.fori_loop(0, SEQ // 32, norm_rows, 0)
    relative_columns(at, normed, GROUPS[:2], rel)
    relative_columns(at, normed, GROUPS[2:], rest)
    project_rows(rel[...], pieces, None, acc)
    copies[1].wait()
    project_heads(at, g, pieces, GROUPS[:2], attn_grad)


def first_stage(at, layer_inputs, out_grads, gain, groups):
    pieces = [array for pair in groups for array in pair]
    return pl.pallas_call(
        first_body,
        in_specs=[SMEM, HBM, HBM] + [VMEM] * (1 + 8),
        out_specs=[VMEM] * 3,
        out_shape=[
            jax.ShapeDtypeStruct((SEQ, WIDTH), f32),
            jax.ShapeDtypeStruct((SEQ, QW), bf16),
            jax.ShapeDtypeStruct((SEQ, QW), bf16),
        ],
        scratch_shapes=[
            pltpu.VMEM((SEQ, D), bf16),
            pltpu.VMEM((SEQ, D), bf16),
            pltpu.VMEM((SEQ, D), bf16),
            pltpu.VMEM((SEQ, QW), bf16),
            pltpu.SemaphoreType.DMA((2,)),
        ],
        compiler_params=limit(24),
        name="first_stage",
    )(at, layer_inputs, out_grads, gain, *pieces)


def more_body(at, g_all, acc_in, attn_in, rest, *refs):
    pieces, (acc, attn_grad, g, sems) = (refs[:4], refs[4:])
    copy = pltpu.make_async_copy(g_all.at[0, at[3]], g, sems.at[0])
    copy.start()
    attn_grad[...] = attn_in[...]
    project_rows(rest[:, : 4 * TILE], pieces, acc_in, acc)
    copy.wait()
    project_heads(at, g, pieces, GROUPS[2:3], attn_grad)


def more_stage(at, out_grads, acc, attn_grad, rest, group):
    return pl.pallas_call(
        more_body,
        in_specs=[SMEM, HBM] + [VMEM] * 7,
        out_specs=[VMEM] * 2,
        out_shape=[jax.ShapeDtypeStruct((SEQ, WIDTH), f32), jax.ShapeDtypeStruct((SEQ, QW), bf16)],
        scratch_shapes=[pltpu.VMEM((SEQ, D), bf16), pltpu.SemaphoreType.DMA((1,))],
        compiler_params=limit(20),
        name="more_stage",
    )(at, out_grads, acc, attn_grad, rest, *group)


def whole_spec(shape):
    return pl.BlockSpec(shape, lambda i, at: (0,) * len(shape))


def first_half_lanes(rows):
    lanes = lax.broadcasted_iota(jnp.int32, (rows, TILE), 1)
    return lax.rem(lanes, HEAD_DIM) < HEAD_DIM // 2


def rope(u, cosine, sine):
    turned = jnp.where(
        first_half_lanes(u.shape[0]), -pltpu.roll(u, TILE - 32, 1), pltpu.roll(u, 32, 1)
    )
    return u * cosine + turned * sine


def unrope(u, cosine, sine):
    v = u * sine
    turned = jnp.where(
        first_half_lanes(u.shape[0]), -pltpu.roll(v, TILE - 32, 1), pltpu.roll(v, 32, 1)
    )
    return u * cosine - turned


def lower_lanes(rows):
    return lax.broadcasted_iota(jnp.int32, (rows, TILE), 1) < HEAD_DIM


def key_half(block, odd):
    wide = block.astype(f32)
    if odd:
        wide = pltpu.roll(wide, HEAD_DIM, 1)
    return jnp.where(lower_lanes(block.shape[0]), wide, 0.0)


def lane_block(block):
    return pl.ds(pl.multiple_of(block * TILE, TILE), TILE)


def stacked_heads(source, tile_rows, group):
    parts = []
    for pair in range(2):
        block = source[tile_rows, lane_block(2 * group + pair)]
        parts += [block, pltpu.roll(block.astype(f32), HEAD_DIM, 1).astype(bf16)]
    return jnp.concatenate(parts, axis=0)


def attention_tile(qkv, attn_grad, tile, both, odd, grad_q, grad_k, grad_v, fresh):
    count = (tile + 1) * TILE
    tile_rows = slice(tile * TILE, count)
    group = 2 * both + odd
    keys = (key_half(qkv[:count, lane_block(8 + both)], odd) * 0.125).astype(bf16)
    values = key_half(qkv[:count, lane_block(10 + both)], odd).astype(bf16)
    queries = stacked_heads(qkv, tile_rows, group)
    grads = stacked_heads(attn_grad, tile_rows, group)
    weights = jnp.exp(nt(keys, queries))
    key_ids = lax.broadcasted_iota(jnp.int32, (TILE, 4 * TILE), 0)
    query_ids = lax.rem(lax.broadcasted_iota(jnp.int32, (TILE, 4 * TILE), 1), TILE)
    last = jnp.where(key_ids <= query_ids, weights[tile * TILE :], 0.0)
    weights = last if tile == 0 else jnp.concatenate([weights[: tile * TILE], last], axis=0)
    probs = weights * (1.0 / jnp.sum(weights, axis=0, keepdims=True))
    grad_probs = nt(values, grads)
    delta = jnp.sum(probs * grad_probs, axis=0, keepdims=True)
    grad_scores = (probs * (grad_probs - delta)).astype(bf16)
    value_part = nn(probs.astype(bf16), grads)
    key_part = nn(grad_scores, queries) * 0.125
    if fresh:
        grad_v[group, :count, :] = value_part
        grad_k[group, :count, :] = key_part
    else:
        grad_v[group, :count, :] += value_part
        grad_k[group, :count, :] += key_part
    turned = tn(keys, grad_scores)[:HEAD_DIM]
    for pair in range(2):
        both = jnp.concatenate(
            [turned[:, (2 * pair + i) * TILE : (2 * pair + i + 1) * TILE] for i in range(2)], axis=0
        )
        grad_q(2 * group + pair, both.T)


def finish_rows(at, rows, grad_proj, pieces, x, g, gain, grad_normed, out):
    core = at[2]
    for n, chip in enumerate(chips_of(at, GROUPS)):
        both = jnp.concatenate(
            [
                jnp.concatenate([qkv_block(piece, j) for j in range(3)], axis=1)
                for piece in pieces[2 * n : 2 * n + 2]
            ],
            axis=0,
        )
        part = nt(grad_proj[...], both)
        for half, place in ((0, core), (1, 1 - core)):
            cols = pl.ds(pl.multiple_of((chip * 2 + place) * TILE, TILE), TILE)
            grad_normed[:, cols] = part[:, half * TILE : (half + 1) * TILE]

    def norm_rows(i, carry):
        here = pl.ds(pl.multiple_of(i * 16, 16), 16)
        wide = x[here, :].astype(f32)
        inv = inverse_rms(wide)
        scaled = grad_normed[here, :] * gain[...]
        inner = jnp.mean(scaled * wide, axis=-1, keepdims=True)
        result = g[here, :].astype(f32) + inv * scaled - wide * (inv * inv * inv * inner)
        out[here, :] = result.astype(bf16)
        return carry

    lax.fori_loop(0, rows // 16, norm_rows, 0)


def join_keys(grad_k, grad_v, rows, cosine, sine, grad_proj):
    lower = lower_lanes(TILE)
    for pair in range(2):
        for first in range(rows[0], rows[1], TILE):
            here = slice(first, first + TILE)
            there = slice(first - rows[0], first - rows[0] + TILE)
            k = jnp.where(
                lower,
                grad_k[2 * pair, here, :],
                pltpu.roll(grad_k[2 * pair + 1, here, :], HEAD_DIM, 1),
            )
            v = jnp.where(
                lower,
                grad_v[2 * pair, here, :],
                pltpu.roll(grad_v[2 * pair + 1, here, :], HEAD_DIM, 1),
            )
            at_key = QW + pair * TILE
            grad_proj[there, at_key : at_key + TILE] = unrope(
                k, cosine[here, :], sine[here, :]
            ).astype(bf16)
            grad_proj[there, at_key + 2 * TILE : at_key + 3 * TILE] = v.astype(bf16)


def store_query_grads(grad_proj, there, cosine, sine):
    def store(block, value):
        grad_proj[there, lane_block(block)] = unrope(value, cosine, sine).astype(bf16)

    return store


def second_body(
    at, x_all, g_all, gain, cosine, sine, acc_in, attn_in, rest, *refs
):
    pieces, (out, qkv_first, attn_first, grad_k_first, grad_v_first) = (refs[:16], refs[16:21])
    x, g, acc, attn_grad, qkv, grad_k, grad_v, grad_proj, grad_normed, sems = refs[21:]
    slot = at[3]
    copies = [
        pltpu.make_async_copy(g_all.at[0, slot], g, sems.at[1]),
        pltpu.make_async_copy(x_all.at[0, slot, pl.ds(TILE, 2 * TILE)], x, sems.at[0]),
    ]
    for copy in copies:
        copy.start()
    attn_grad[...] = attn_in[...]
    project_rows(rest[:, 4 * TILE :], pieces[12:], acc_in, acc)
    for block in range(10):
        cols = slice(block * TILE, (block + 1) * TILE)
        qkv[:, cols] = rope(acc[:, cols], cosine[...], sine[...]).astype(bf16)
    qkv[:, 10 * TILE :] = acc[:, 10 * TILE :].astype(bf16)
    copies[0].wait()
    project_heads(at, g, pieces[12:], GROUPS[3:], attn_grad)

    def two_groups(both, carry):
        for tile in (2, 1):
            here = slice(tile * TILE, (tile + 1) * TILE)
            there = slice((tile - 1) * TILE, tile * TILE)
            store = store_query_grads(grad_proj, there, cosine[here, :], sine[here, :])
            for odd in range(2):
                attention_tile(qkv, attn_grad, tile, both, odd, store, grad_k, grad_v, tile == 2)
        return carry

    lax.fori_loop(0, 2, two_groups, 0)
    join_keys(grad_k, grad_v, (TILE, SEQ), cosine, sine, grad_proj)
    copies[1].wait()
    finish_rows(at, 2 * TILE, grad_proj, pieces, x, g.at[TILE:], gain, grad_normed, out)
    qkv_first[...] = qkv[:TILE, :]
    attn_first[...] = attn_grad[:TILE, :]
    grad_k_first[...] = grad_k[:, :TILE, :]
    grad_v_first[...] = grad_v[:, :TILE, :]


def second_stage(at, layer_inputs, out_grads, gain, tables, acc, attn_grad, rest, groups):
    pieces = [array for pair in groups for array in pair]
    return pl.pallas_call(
        second_body,
        in_specs=[SMEM, HBM, HBM] + [VMEM] * (6 + 16),
        out_specs=[VMEM] * 5,
        out_shape=[
            jax.ShapeDtypeStruct((2 * TILE, D), bf16),
            jax.ShapeDtypeStruct((TILE, WIDTH), bf16),
            jax.ShapeDtypeStruct((TILE, QW), bf16),
            jax.ShapeDtypeStruct((KV_HEADS, TILE, TILE), f32),
            jax.ShapeDtypeStruct((KV_HEADS, TILE, TILE), f32),
        ],
        scratch_shapes=[
            pltpu.VMEM((2 * TILE, D), bf16),
            pltpu.VMEM((SEQ, D), bf16),
            pltpu.VMEM((SEQ, WIDTH), f32),
            pltpu.VMEM((SEQ, QW), bf16),
            pltpu.VMEM((SEQ, WIDTH), bf16),
            pltpu.VMEM((KV_HEADS, SEQ, TILE), f32),
            pltpu.VMEM((KV_HEADS, SEQ, TILE), f32),
            pltpu.VMEM((2 * TILE, WIDTH), bf16),
            pltpu.VMEM((2 * TILE, D), f32),
            pltpu.SemaphoreType.DMA((2,)),
        ],
        compiler_params=limit(24),
        name="second_stage",
    )(at, layer_inputs, out_grads, gain, *tables, acc, attn_grad, rest, *pieces)


def third_body(
    at, x_all, g_all, gain, cosine, sine, qkv, attn_grad, grad_k_in, grad_v_in, *refs
):
    pieces, (out, x, g, grad_k, grad_v, grad_proj, grad_normed, sems) = (refs[:16], refs[16:])
    slot = at[3]
    copies = [
        pltpu.make_async_copy(x_all.at[0, slot, pl.ds(0, TILE)], x, sems.at[0]),
        pltpu.make_async_copy(g_all.at[0, slot, pl.ds(0, TILE)], g, sems.at[1]),
    ]
    for copy in copies:
        copy.start()
    grad_k[...] = grad_k_in[...]
    grad_v[...] = grad_v_in[...]
    here = slice(0, TILE)
    store = store_query_grads(grad_proj, here, cosine[here, :], sine[here, :])

    def two_groups(both, carry):
        for odd in range(2):
            attention_tile(qkv, attn_grad, 0, both, odd, store, grad_k, grad_v, False)
        return carry

    lax.fori_loop(0, 2, two_groups, 0)
    join_keys(grad_k, grad_v, (0, TILE), cosine, sine, grad_proj)
    for copy in copies:
        copy.wait()
    finish_rows(at, TILE, grad_proj, pieces, x, g, gain, grad_normed, out)


def third_stage(at, layer_inputs, out_grads, gain, tables, carried, groups):
    pieces = [array for pair in groups for array in pair]
    return pl.pallas_call(
        third_body,
        in_specs=[SMEM, HBM, HBM] + [VMEM] * (7 + 16),
        out_specs=VMEM,
        out_shape=jax.ShapeDtypeStruct((TILE, D), bf16),
        scratch_shapes=[
            pltpu.VMEM((TILE, D), bf16),
            pltpu.VMEM((TILE, D), bf16),
            pltpu.VMEM((KV_HEADS, TILE, TILE), f32),
            pltpu.VMEM((KV_HEADS, TILE, TILE), f32),
            pltpu.VMEM((TILE, WIDTH), bf16),
            pltpu.VMEM((TILE, D), f32),
            pltpu.SemaphoreType.DMA((2,)),
        ],
        compiler_params=limit(24),
        name="third_stage",
    )(at, layer_inputs, out_grads, gain, *tables, *carried, *pieces)


def weight_body(at, x_all, p_all, a_all, e_all, gain, sent, kept, x, p, a, e, inv, sems):
    step = pl.program_id(0)
    slot = at[3]
    copies = [
        pltpu.make_async_copy(whole.at[0, slot], part, sems.at[n])
        for n, (whole, part) in enumerate(((x_all, x), (p_all, p), (a_all, a), (e_all, e)))
    ]

    @pl.when(step == 0)
    def _():
        for copy in copies:
            copy.start()
        copies[0].wait()

        def norm_rows(i, carry):
            rows = pl.ds(pl.multiple_of(i * 32, 32), 32)
            inv[rows, :] = jnp.broadcast_to(inverse_rms(x[rows, :].astype(f32)), (32, TILE))
            return carry

        lax.fori_loop(0, SEQ // 32, norm_rows, 0)
        for copy in copies[1:]:
            copy.wait()

    flip = lax.rem(step, 2)
    x_at = at[0] + flip - 2 * at[0] * flip
    chip = x_at * 4 + lax.rem(at[1] + step // 2, 4)
    cols = pl.ds(pl.multiple_of(chip * 2 * TILE, 2 * TILE), 2 * TILE)
    scale = jnp.concatenate([inv[...], inv[...]], axis=1)
    normed = (x[:, cols].astype(f32) * scale * gain[:, cols]).astype(bf16)
    part = tn(normed, p[...])
    core_zero = at[2] == 0
    for j in range(3):
        where = slice(j * TILE, (j + 1) * TILE)
        top = part[:TILE, j * BLOCK : (j + 1) * BLOCK].astype(bf16)
        low = part[TILE:, j * BLOCK : (j + 1) * BLOCK].astype(bf16)
        kept[0, where, :] = jnp.where(core_zero, top, low)
        sent[0, where, :] = jnp.where(core_zero, low, top)
    heads = a[:, pl.ds(pl.multiple_of(chip * TILE, TILE), TILE)]
    part = tn(heads, e[...])
    for j in range(4):
        where = slice(Q_ROWS + j * HEAD_DIM, Q_ROWS + (j + 1) * HEAD_DIM)
        top = part[:HEAD_DIM, j * BLOCK : (j + 1) * BLOCK].astype(bf16)
        low = part[HEAD_DIM:, j * BLOCK : (j + 1) * BLOCK].astype(bf16)
        kept[0, where, :] = jnp.where(core_zero, top, low)
        sent[0, where, :] = jnp.where(core_zero, low, top)


def weight_stage(at, layer_inputs, proj_grads, attn_stash, out_grads, gain):
    block = pl.BlockSpec((1, PIECE, BLOCK), lambda i, at: (lax.rem(i, 2) * 4 + i // 2, 0, 0))
    shape = jax.ShapeDtypeStruct((8, PIECE, BLOCK), bf16)
    return pl.pallas_call(
        weight_body,
        grid_spec=pltpu.PrefetchScalarGridSpec(
            num_scalar_prefetch=1,
            grid=(8,),
            in_specs=[HBM] * 4 + [whole_spec((1, D))],
            out_specs=[block, block],
            scratch_shapes=[
                pltpu.VMEM((SEQ, D), bf16),
                pltpu.VMEM((SEQ, WIDTH), bf16),
                pltpu.VMEM((SEQ, QW), bf16),
                pltpu.VMEM((SEQ, D), bf16),
                pltpu.VMEM((SEQ, TILE), f32),
                pltpu.SemaphoreType.DMA((4,)),
            ],
        ),
        out_shape=[shape, shape],
        compiler_params=limit(56),
        name="weight_stage",
    )(at, layer_inputs, proj_grads, attn_stash, out_grads, gain)


def wide(array):
    return array.astype(f32)


def prepare_body(kept, received, up, down, k, r, sems):
    copies = []
    for n in range(2):
        far = (4 * n + 2, pl.ds(0, Q_ROWS))
        copies.append(pltpu.make_async_copy(kept.at[far], k.at[n], sems.at[2 * n]))
        copies.append(pltpu.make_async_copy(received.at[far], r.at[n], sems.at[2 * n + 1]))
    for copy in copies:
        copy.start()
    for copy in copies:
        copy.wait()
    for n, out in enumerate((up, down)):
        out[...] = (wide(k[n]) + wide(r[n])).astype(bf16)


def prepare_stage(kept, received):
    shape = jax.ShapeDtypeStruct((Q_ROWS, BLOCK), bf16)
    return pl.pallas_call(
        prepare_body,
        in_specs=[HBM] * 2,
        out_specs=[VMEM] * 2,
        out_shape=[shape, shape],
        scratch_shapes=[
            pltpu.VMEM((2, Q_ROWS, BLOCK), bf16),
            pltpu.VMEM((2, Q_ROWS, BLOCK), bf16),
            pltpu.SemaphoreType.DMA((4,)),
        ],
        compiler_params=limit(10),
        name="prepare",
    )(kept, received)


def final_body(mine, last, qkv):
    total = mine[...] + last[...].astype(f32)
    for j in range(3):
        qkv[0, :, j * BLOCK : (j + 1) * BLOCK] = total[j * TILE : (j + 1) * TILE]


def final_sum(mine, last):
    return pl.pallas_call(
        final_body,
        in_specs=[VMEM] * 2,
        out_specs=VMEM,
        out_shape=jax.ShapeDtypeStruct((1, TILE, WIDTH), f32),
        compiler_params=limit(6),
        name="final_sum",
    )(mine, last)


def out_body(mine, far, above, below, out):
    total = mine[...] + wide(far[...]) + wide(above[...]) + wide(below[...])
    for j in range(4):
        out[0, :, j * BLOCK : (j + 1) * BLOCK] = total[j * HEAD_DIM : (j + 1) * HEAD_DIM]


def out_total(*arrays):
    return pl.pallas_call(
        out_body,
        in_specs=[VMEM] * 4,
        out_specs=VMEM,
        out_shape=jax.ShapeDtypeStruct((1, HEAD_DIM, D), f32),
        compiler_params=limit(6),
        name="out_total",
    )(*arrays)


def scattered(sent, kept):
    received = passed_along(sent, "core", 1)
    across = (wide(kept[4:, Q_ROWS:]) + wide(received[4:, Q_ROWS:])).astype(bf16)
    across = passed_along(across, "x_hi", 1)
    up, down = prepare_stage(kept, received)
    up = wide(from_below(up))
    down = wide(from_above(down))

    def qkv_sum(dx, dy):
        at = 4 * dx + dy
        return wide(kept[at, :Q_ROWS]) + wide(received[at, :Q_ROWS])

    def out_sum(dy):
        return wide(kept[dy, Q_ROWS:]) + wide(received[dy, Q_ROWS:]) + wide(across[dy])

    above = jnp.concatenate([qkv_sum(0, 1) + up, qkv_sum(1, 1)])
    below = jnp.concatenate([qkv_sum(0, 3), qkv_sum(1, 3) + down])
    above = wide(from_below(above.astype(bf16)))
    below = wide(from_above(below.astype(bf16)))
    out_far = passed_along(out_sum(2).astype(bf16), "y", 2)
    out_above = from_below(out_sum(1).astype(bf16))
    out_below = from_above(out_sum(3).astype(bf16))
    kept_rows = qkv_sum(0, 0) + above[:Q_ROWS] + below[:Q_ROWS]
    sent_rows = qkv_sum(1, 0) + above[Q_ROWS:] + below[Q_ROWS:]
    last = passed_along(sent_rows.astype(bf16), "x_hi", 1)
    return (final_sum(kept_rows, last), out_total(out_sum(0), out_far, out_above, out_below))


def local_step(
    layer_inputs, out_grads, attn_stash, proj_grads, w_qkv, w_out, norm_gain, b_sched, w_sched
):
    tables = rope_tables(SEQ)
    place = [lax.axis_index(name) for name in FSDP]
    at_b = jnp.stack([*place, b_sched[0]]).astype(jnp.int32)
    at_w = jnp.stack([*place, w_sched[0]]).astype(jnp.int32)
    groups = gathered_groups(packed_shard(w_qkv, w_out))
    sent, kept = weight_stage(at_w, layer_inputs, proj_grads, attn_stash, out_grads, norm_gain)
    acc, attn_grad, rest = first_stage(at_b, layer_inputs, out_grads, norm_gain, groups[:2])
    acc, attn_grad = more_stage(at_b, out_grads, acc, attn_grad, rest, groups[2])
    grads = scattered(sent, kept)
    second, *carried = second_stage(
        at_b, layer_inputs, out_grads, norm_gain, tables, acc, attn_grad, rest, groups
    )
    second = passed_along(second, SECTION, -1)
    first = third_stage(at_b, layer_inputs, out_grads, norm_gain, tables, carried, groups)
    first = passed_along(first, SECTION, -1)
    sent_back = jnp.concatenate([first, second], axis=0)
    return (sent_back[None], *grads)


def solution(mesh):
    finer = Mesh(mesh.devices.reshape(mesh.shape["section"] // 2, 2, 2, 4, 2), SECTION + FSDP)
    return jax.shard_map(
        local_step,
        mesh=finer,
        in_specs=(
            P(SECTION, None, FSDP, None),
            P(SECTION, None, FSDP, None),
            P(SECTION, None, FSDP, None),
            P(SECTION, None, FSDP, None),
            P(SECTION, FSDP, None),
            P(SECTION, FSDP, None),
            P(SECTION, None),
            P(SECTION),
            P(SECTION),
        ),
        out_specs=(P(SECTION, FSDP, None), P(SECTION, FSDP, None), P(SECTION, FSDP, None)),
        check_vma=False,
    )
```

```python
import jax
import jax.numpy as jnp
import numpy as np
from jax import lax
from jax.experimental import pallas as pl
from jax.experimental.pallas import tpu as pltpu
from jax.sharding import Mesh
from jax.sharding import PartitionSpec as P


HEAD_DIM = 64
KV_HEADS = 4
SECTION = ("z", "x_lo")
FSDP = ("x_hi", "y", "core")
SEQ = 384
D = 2048
QW = 1024
WIDTH = 1536
BLOCK = 512
Q_ROWS = 384
PIECE = 640
TILE = 128


rms_eps = 1e-05
rope_base = 500000.0
f32 = jnp.float32
bf16 = jnp.bfloat16

GROUPS = (((0, 0), (1, 0)), ((0, 1), (0, 3)), ((1, 1), (1, 3)), ((0, 2), (1, 2)))

VMEM = pl.BlockSpec(memory_space=pltpu.VMEM)
SMEM = pl.BlockSpec(memory_space=pltpu.SMEM)
HBM = pl.BlockSpec(memory_space=pltpu.HBM)


def passed_along(array, axis, by):
    size = lax.axis_size(axis)
    return lax.ppermute(array, axis, [(i, (i + by) % size) for i in range(size)])


def from_above(array):
    return passed_along(array, "y", -1)


def from_below(array):
    return passed_along(array, "y", 1)


def limit(mebibytes):
    return pltpu.CompilerParams(vmem_limit_bytes=mebibytes << 20)


def pack_body(qkv, out, packed):
    for j in range(3):
        packed[j * TILE : (j + 1) * TILE, :] = qkv[0, :, j * BLOCK : (j + 1) * BLOCK]
    for j in range(4):
        packed[Q_ROWS + j * HEAD_DIM : Q_ROWS + (j + 1) * HEAD_DIM, :] = out[
            0, :, j * BLOCK : (j + 1) * BLOCK
        ]


def packed_shard(qkv, out):
    return pl.pallas_call(
        pack_body,
        in_specs=[VMEM, VMEM],
        out_specs=VMEM,
        out_shape=jax.ShapeDtypeStruct((PIECE, BLOCK), bf16),
        compiler_params=limit(4),
        name="pack",
    )(qkv, out)


def gathered_groups(shard):
    other = passed_along(shard, "x_hi", 1)
    above, below = (from_above(shard), from_below(shard))
    above_other = from_above(other)
    below_other = from_below(other)
    far = from_above(above)
    far_other = from_below(below_other)

    def with_peer(array):
        return (array, passed_along(array, "core", 1))

    return (
        (*with_peer(shard), *with_peer(other)),
        (*with_peer(above), *with_peer(below)),
        (*with_peer(above_other), *with_peer(below_other)),
        (*with_peer(far), *with_peer(far_other)),
    )


def rope_tables(length):
    fine = 16
    half = HEAD_DIM // 2
    frequency = rope_base ** (-2.0 * np.arange(half) / HEAD_DIM)

    def table(function, positions):
        return jnp.asarray(function(positions[:, None] * frequency[None, :]), f32)

    steps = (np.arange(length // fine) * fine, np.arange(fine))
    cosines = [table(np.cos, step) for step in steps]
    sines = [table(np.sin, step) for step in steps]

    def outer(first, second):
        return first[:, None, :] * second[None, :, :]

    cosine = outer(cosines[0], cosines[1]) - outer(sines[0], sines[1])
    sine = outer(sines[0], cosines[1]) + outer(cosines[0], sines[1])
    return tuple(
        jnp.concatenate([part.reshape(length, half)] * 4, axis=1) for part in (cosine, sine)
    )


def nt(lhs, rhs):
    return lax.dot_general(lhs, rhs, (((1,), (1,)), ((), ())), preferred_element_type=f32)


def tn(lhs, rhs):
    return lax.dot_general(lhs, rhs, (((0,), (0,)), ((), ())), preferred_element_type=f32)


def nn(lhs, rhs):
    return jnp.dot(lhs, rhs, preferred_element_type=f32)


def chip_of(at, dx, dy):
    x_at = at[0] if dx == 0 else 1 - at[0]
    return x_at * 4 + lax.rem(at[1] + dy, 4)


def qkv_block(piece, j):
    return piece[j * TILE : (j + 1) * TILE, :]


def out_block(piece, j):
    return piece[Q_ROWS + j * HEAD_DIM : Q_ROWS + (j + 1) * HEAD_DIM, :]


def inverse_rms(rows):
    return lax.rsqrt(jnp.mean(rows * rows, axis=-1, keepdims=True) + rms_eps)


def chips_of(at, keys):
    return [chip_of(at, dx, dy) for pair in keys for dx, dy in pair]


def relative_columns(at, normed, keys, rel):
    core = at[2]
    for n, chip in enumerate(chips_of(at, keys)):
        for half, place in ((0, core), (1, 1 - core)):
            cols = pl.ds(pl.multiple_of((chip * 2 + place) * TILE, TILE), TILE)
            rel[:, (2 * n + half) * TILE : (2 * n + half + 1) * TILE] = normed[:, cols]


def project_rows(rel, pieces, acc_init, acc):
    for j in range(3):
        rows = [qkv_block(piece, j) for piece in pieces]
        cols = slice(j * BLOCK, (j + 1) * BLOCK)
        total = nn(rel, jnp.concatenate(rows, axis=0))
        if acc_init is not None:
            total = total + acc_init[:, cols]
        acc[:, cols] = total


def project_heads(at, upstream, pieces, keys, attn_grad):
    core = at[2]
    heads = None
    for j in range(4):
        rows = [out_block(piece, j) for piece in pieces]
        part = nt(upstream[:, j * BLOCK : (j + 1) * BLOCK], jnp.concatenate(rows, axis=0))
        heads = part if heads is None else heads + part
    for n, chip in enumerate(chips_of(at, keys)):
        block = heads[:, n * TILE : (n + 1) * TILE]
        block = jnp.where(core == 0, block, pltpu.roll(block, HEAD_DIM, 1))
        attn_grad[:, pl.ds(pl.multiple_of(chip * TILE, TILE), TILE)] = block.astype(bf16)


def first_body(
    at, x_all, g_all, gain, *refs
):
    pieces, (acc, attn_grad, rest, x, g, normed, rel, sems) = (refs[:8], refs[8:])
    copies = [
        pltpu.make_async_copy(x_all.at[0, at[3]], x, sems.at[0]),
        pltpu.make_async_copy(g_all.at[0, at[3]], g, sems.at[1]),
    ]
    for copy in copies:
        copy.start()
    copies[0].wait()

    def norm_rows(i, carry):
        rows = pl.ds(pl.multiple_of(i * 32, 32), 32)
        wide = x[rows, :].astype(f32)
        normed[rows, :] = (wide * inverse_rms(wide) * gain[...]).astype(bf16)
        return carry

    lax.fori_loop(0, SEQ // 32, norm_rows, 0)
    relative_columns(at, normed, GROUPS[:2], rel)
    relative_columns(at, normed, GROUPS[2:], rest)
    project_rows(rel[...], pieces, None, acc)
    copies[1].wait()
    project_heads(at, g, pieces, GROUPS[:2], attn_grad)


def first_stage(at, layer_inputs, out_grads, gain, groups):
    pieces = [array for pair in groups for array in pair]
    return pl.pallas_call(
        first_body,
        in_specs=[SMEM, HBM, HBM] + [VMEM] * (1 + 8),
        out_specs=[VMEM] * 3,
        out_shape=[
            jax.ShapeDtypeStruct((SEQ, WIDTH), f32),
            jax.ShapeDtypeStruct((SEQ, QW), bf16),
            jax.ShapeDtypeStruct((SEQ, QW), bf16),
        ],
        scratch_shapes=[
            pltpu.VMEM((SEQ, D), bf16),
            pltpu.VMEM((SEQ, D), bf16),
            pltpu.VMEM((SEQ, D), bf16),
            pltpu.VMEM((SEQ, QW), bf16),
            pltpu.SemaphoreType.DMA((2,)),
        ],
        compiler_params=limit(16),
        name="first_stage",
    )(at, layer_inputs, out_grads, gain, *pieces)


def more_body(at, g_all, acc_in, attn_in, rest, *refs):
    pieces, (acc, attn_grad, g, sems) = (refs[:4], refs[4:])
    copy = pltpu.make_async_copy(g_all.at[0, at[3]], g, sems.at[0])
    copy.start()
    attn_grad[...] = attn_in[...]
    project_rows(rest[:, : 4 * TILE], pieces, acc_in, acc)
    copy.wait()
    project_heads(at, g, pieces, GROUPS[2:3], attn_grad)


def more_stage(at, out_grads, acc, attn_grad, rest, group):
    return pl.pallas_call(
        more_body,
        in_specs=[SMEM, HBM] + [VMEM] * 7,
        out_specs=[VMEM] * 2,
        out_shape=[jax.ShapeDtypeStruct((SEQ, WIDTH), f32), jax.ShapeDtypeStruct((SEQ, QW), bf16)],
        scratch_shapes=[pltpu.VMEM((SEQ, D), bf16), pltpu.SemaphoreType.DMA((1,))],
        compiler_params=limit(10),
        name="more_stage",
    )(at, out_grads, acc, attn_grad, rest, *group)


def whole_spec(shape):
    return pl.BlockSpec(shape, lambda i, at: (0,) * len(shape))


def first_half_lanes(rows):
    lanes = lax.broadcasted_iota(jnp.int32, (rows, TILE), 1)
    return lax.rem(lanes, HEAD_DIM) < HEAD_DIM // 2


def rope(u, cosine, sine):
    turned = jnp.where(
        first_half_lanes(u.shape[0]), -pltpu.roll(u, TILE - 32, 1), pltpu.roll(u, 32, 1)
    )
    return u * cosine + turned * sine


def unrope(u, cosine, sine):
    v = u * sine
    turned = jnp.where(
        first_half_lanes(u.shape[0]), -pltpu.roll(v, TILE - 32, 1), pltpu.roll(v, 32, 1)
    )
    return u * cosine - turned


def lower_lanes(rows):
    return lax.broadcasted_iota(jnp.int32, (rows, TILE), 1) < HEAD_DIM


def key_half(block, odd):
    wide = block.astype(f32)
    if odd:
        wide = pltpu.roll(wide, HEAD_DIM, 1)
    return jnp.where(lower_lanes(block.shape[0]), wide, 0.0)


def lane_block(block):
    if isinstance(block, int):
        return slice(block * TILE, (block + 1) * TILE)
    return pl.ds(pl.multiple_of(block * TILE, TILE), TILE)


def stacked_heads(source, tile_rows, group):
    parts = []
    for pair in range(2):
        block = source[tile_rows, lane_block(2 * group + pair)]
        parts += [block, pltpu.roll(block.astype(f32), HEAD_DIM, 1).astype(bf16)]
    return jnp.concatenate(parts, axis=0)


def attention_tile(qkv, attn_grad, tile, both, odd, grad_q, grad_k, grad_v, fresh):
    count = (tile + 1) * TILE
    tile_rows = slice(tile * TILE, count)
    group = 2 * both + odd
    keys = (key_half(qkv[:count, lane_block(8 + both)], odd) * 0.125).astype(bf16)
    values = key_half(qkv[:count, lane_block(10 + both)], odd).astype(bf16)
    queries = stacked_heads(qkv, tile_rows, group)
    grads = stacked_heads(attn_grad, tile_rows, group)
    weights = jnp.exp(nt(keys, queries))
    key_ids = lax.broadcasted_iota(jnp.int32, (TILE, 4 * TILE), 0)
    query_ids = lax.rem(lax.broadcasted_iota(jnp.int32, (TILE, 4 * TILE), 1), TILE)
    last = jnp.where(key_ids <= query_ids, weights[tile * TILE :], 0.0)
    weights = last if tile == 0 else jnp.concatenate([weights[: tile * TILE], last], axis=0)
    probs = weights * (1.0 / jnp.sum(weights, axis=0, keepdims=True))
    grad_probs = nt(values, grads)
    delta = jnp.sum(probs * grad_probs, axis=0, keepdims=True)
    grad_scores = (probs * (grad_probs - delta)).astype(bf16)
    value_part = nn(probs.astype(bf16), grads)
    key_part = nn(grad_scores, queries) * 0.125
    if fresh:
        grad_v[group, :count, :] = value_part
        grad_k[group, :count, :] = key_part
    else:
        grad_v[group, :count, :] += value_part
        grad_k[group, :count, :] += key_part
    turned = tn(keys, grad_scores)[:HEAD_DIM]
    for pair in range(2):
        both = jnp.concatenate(
            [turned[:, (2 * pair + i) * TILE : (2 * pair + i + 1) * TILE] for i in range(2)], axis=0
        )
        grad_q(2 * group + pair, both.T)


def finish_rows(at, rows, grad_proj, pieces, x, g, gain, grad_normed, out):
    core = at[2]
    for n, chip in enumerate(chips_of(at, GROUPS)):
        both = jnp.concatenate(
            [
                jnp.concatenate([qkv_block(piece, j) for j in range(3)], axis=1)
                for piece in pieces[2 * n : 2 * n + 2]
            ],
            axis=0,
        )
        part = nt(grad_proj[...], both)
        for half, place in ((0, core), (1, 1 - core)):
            cols = pl.ds(pl.multiple_of((chip * 2 + place) * TILE, TILE), TILE)
            grad_normed[:, cols] = part[:, half * TILE : (half + 1) * TILE]

    def norm_rows(i, carry):
        here = pl.ds(pl.multiple_of(i * 16, 16), 16)
        wide = x[here, :].astype(f32)
        inv = inverse_rms(wide)
        scaled = grad_normed[here, :] * gain[...]
        inner = jnp.mean(scaled * wide, axis=-1, keepdims=True)
        result = g[here, :].astype(f32) + inv * scaled - wide * (inv * inv * inv * inner)
        out[here, :] = result.astype(bf16)
        return carry

    lax.fori_loop(0, rows // 16, norm_rows, 0)


def join_keys(grad_k, grad_v, rows, cosine, sine, grad_proj):
    lower = lower_lanes(TILE)
    for pair in range(2):
        for first in range(rows[0], rows[1], TILE):
            here = slice(first, first + TILE)
            there = slice(first - rows[0], first - rows[0] + TILE)
            k = jnp.where(
                lower,
                grad_k[2 * pair, here, :],
                pltpu.roll(grad_k[2 * pair + 1, here, :], HEAD_DIM, 1),
            )
            v = jnp.where(
                lower,
                grad_v[2 * pair, here, :],
                pltpu.roll(grad_v[2 * pair + 1, here, :], HEAD_DIM, 1),
            )
            at_key = QW + pair * TILE
            grad_proj[there, at_key : at_key + TILE] = unrope(
                k, cosine[here, :], sine[here, :]
            ).astype(bf16)
            grad_proj[there, at_key + 2 * TILE : at_key + 3 * TILE] = v.astype(bf16)


def store_query_grads(grad_proj, there, cosine, sine):
    def store(block, value):
        grad_proj[there, lane_block(block)] = unrope(value, cosine, sine).astype(bf16)

    return store


def second_body(
    at, x_all, g_all, gain, cosine, sine, acc_in, attn_in, rest, *refs
):
    pieces, (out, qkv_first, attn_first, grad_k_first, grad_v_first) = (refs[:16], refs[16:21])
    x, g, acc, attn_grad, qkv, grad_k, grad_v, grad_proj, grad_normed, sems = refs[21:]
    slot = at[3]
    copies = [
        pltpu.make_async_copy(g_all.at[0, slot], g, sems.at[1]),
        pltpu.make_async_copy(x_all.at[0, slot, pl.ds(TILE, 2 * TILE)], x, sems.at[0]),
    ]
    for copy in copies:
        copy.start()
    attn_grad[...] = attn_in[...]
    project_rows(rest[:, 4 * TILE :], pieces[12:], acc_in, acc)
    for block in range(10):
        cols = slice(block * TILE, (block + 1) * TILE)
        qkv[:, cols] = rope(acc[:, cols], cosine[...], sine[...]).astype(bf16)
    qkv[:, 10 * TILE :] = acc[:, 10 * TILE :].astype(bf16)
    copies[0].wait()
    project_heads(at, g, pieces[12:], GROUPS[3:], attn_grad)

    def two_groups(both, carry):
        for tile in (2, 1):
            here = slice(tile * TILE, (tile + 1) * TILE)
            there = slice((tile - 1) * TILE, tile * TILE)
            store = store_query_grads(grad_proj, there, cosine[here, :], sine[here, :])
            for odd in range(2):
                attention_tile(qkv, attn_grad, tile, both, odd, store, grad_k, grad_v, tile == 2)
        return carry

    lax.fori_loop(0, 2, two_groups, 0)
    join_keys(grad_k, grad_v, (TILE, SEQ), cosine, sine, grad_proj)
    copies[1].wait()
    finish_rows(at, 2 * TILE, grad_proj, pieces, x, g.at[TILE:], gain, grad_normed, out)
    qkv_first[...] = qkv[:TILE, :]
    attn_first[...] = attn_grad[:TILE, :]
    grad_k_first[...] = grad_k[:, :TILE, :]
    grad_v_first[...] = grad_v[:, :TILE, :]


def second_stage(at, layer_inputs, out_grads, gain, tables, acc, attn_grad, rest, groups):
    pieces = [array for pair in groups for array in pair]
    return pl.pallas_call(
        second_body,
        in_specs=[SMEM, HBM, HBM] + [VMEM] * (6 + 16),
        out_specs=[VMEM] * 5,
        out_shape=[
            jax.ShapeDtypeStruct((2 * TILE, D), bf16),
            jax.ShapeDtypeStruct((TILE, WIDTH), bf16),
            jax.ShapeDtypeStruct((TILE, QW), bf16),
            jax.ShapeDtypeStruct((KV_HEADS, TILE, TILE), f32),
            jax.ShapeDtypeStruct((KV_HEADS, TILE, TILE), f32),
        ],
        scratch_shapes=[
            pltpu.VMEM((2 * TILE, D), bf16),
            pltpu.VMEM((SEQ, D), bf16),
            pltpu.VMEM((SEQ, WIDTH), f32),
            pltpu.VMEM((SEQ, QW), bf16),
            pltpu.VMEM((SEQ, WIDTH), bf16),
            pltpu.VMEM((KV_HEADS, SEQ, TILE), f32),
            pltpu.VMEM((KV_HEADS, SEQ, TILE), f32),
            pltpu.VMEM((2 * TILE, WIDTH), bf16),
            pltpu.VMEM((2 * TILE, D), f32),
            pltpu.SemaphoreType.DMA((2,)),
        ],
        compiler_params=limit(18),
        name="second_stage",
    )(at, layer_inputs, out_grads, gain, *tables, acc, attn_grad, rest, *pieces)


def third_body(
    at, x_all, g_all, gain, cosine, sine, qkv, attn_grad, grad_k_in, grad_v_in, *refs
):
    pieces, (out, x, g, grad_k, grad_v, grad_proj, grad_normed, sems) = (refs[:16], refs[16:])
    slot = at[3]
    copies = [
        pltpu.make_async_copy(x_all.at[0, slot, pl.ds(0, TILE)], x, sems.at[0]),
        pltpu.make_async_copy(g_all.at[0, slot, pl.ds(0, TILE)], g, sems.at[1]),
    ]
    for copy in copies:
        copy.start()
    grad_k[...] = grad_k_in[...]
    grad_v[...] = grad_v_in[...]
    here = slice(0, TILE)
    store = store_query_grads(grad_proj, here, cosine[here, :], sine[here, :])

    def two_groups(both, carry):
        for odd in range(2):
            attention_tile(qkv, attn_grad, 0, both, odd, store, grad_k, grad_v, False)
        return carry

    lax.fori_loop(0, 2, two_groups, 0)
    join_keys(grad_k, grad_v, (0, TILE), cosine, sine, grad_proj)
    for copy in copies:
        copy.wait()
    finish_rows(at, TILE, grad_proj, pieces, x, g, gain, grad_normed, out)


def third_stage(at, layer_inputs, out_grads, gain, tables, carried, groups):
    pieces = [array for pair in groups for array in pair]
    return pl.pallas_call(
        third_body,
        in_specs=[SMEM, HBM, HBM] + [VMEM] * (7 + 16),
        out_specs=VMEM,
        out_shape=jax.ShapeDtypeStruct((TILE, D), bf16),
        scratch_shapes=[
            pltpu.VMEM((TILE, D), bf16),
            pltpu.VMEM((TILE, D), bf16),
            pltpu.VMEM((KV_HEADS, TILE, TILE), f32),
            pltpu.VMEM((KV_HEADS, TILE, TILE), f32),
            pltpu.VMEM((TILE, WIDTH), bf16),
            pltpu.VMEM((TILE, D), f32),
            pltpu.SemaphoreType.DMA((2,)),
        ],
        compiler_params=limit(10),
        name="third_stage",
    )(at, layer_inputs, out_grads, gain, *tables, *carried, *pieces)


def weight_body(at, x_all, p_all, a_all, e_all, gain, sent, kept, x, p, a, e, inv, sems):
    step = pl.program_id(0)
    slot = at[3]
    copies = [
        pltpu.make_async_copy(whole.at[0, slot], part, sems.at[n])
        for n, (whole, part) in enumerate(((x_all, x), (p_all, p), (a_all, a), (e_all, e)))
    ]

    @pl.when(step == 0)
    def _():
        for copy in copies:
            copy.start()
        copies[0].wait()

        def norm_rows(i, carry):
            rows = pl.ds(pl.multiple_of(i * 32, 32), 32)
            inv[rows, :] = jnp.broadcast_to(inverse_rms(x[rows, :].astype(f32)), (32, TILE))
            return carry

        lax.fori_loop(0, SEQ // 32, norm_rows, 0)
        for copy in copies[1:]:
            copy.wait()

    flip = lax.rem(step, 2)
    x_at = at[0] + flip - 2 * at[0] * flip
    chip = x_at * 4 + lax.rem(at[1] + step // 2, 4)
    cols = pl.ds(pl.multiple_of(chip * 2 * TILE, 2 * TILE), 2 * TILE)
    scale = jnp.concatenate([inv[...], inv[...]], axis=1)
    normed = (x[:, cols].astype(f32) * scale * gain[:, cols]).astype(bf16)
    part = tn(normed, p[...])
    core_zero = at[2] == 0
    for j in range(3):
        where = slice(j * TILE, (j + 1) * TILE)
        top = part[:TILE, j * BLOCK : (j + 1) * BLOCK].astype(bf16)
        low = part[TILE:, j * BLOCK : (j + 1) * BLOCK].astype(bf16)
        kept[0, where, :] = jnp.where(core_zero, top, low)
        sent[0, where, :] = jnp.where(core_zero, low, top)
    heads = a[:, pl.ds(pl.multiple_of(chip * TILE, TILE), TILE)]
    part = tn(heads, e[...])
    for j in range(4):
        where = slice(Q_ROWS + j * HEAD_DIM, Q_ROWS + (j + 1) * HEAD_DIM)
        top = part[:HEAD_DIM, j * BLOCK : (j + 1) * BLOCK].astype(bf16)
        low = part[HEAD_DIM:, j * BLOCK : (j + 1) * BLOCK].astype(bf16)
        kept[0, where, :] = jnp.where(core_zero, top, low)
        sent[0, where, :] = jnp.where(core_zero, low, top)


def weight_stage(at, layer_inputs, proj_grads, attn_stash, out_grads, gain):
    block = pl.BlockSpec((1, PIECE, BLOCK), lambda i, at: (lax.rem(i, 2) * 4 + i // 2, 0, 0))
    shape = jax.ShapeDtypeStruct((8, PIECE, BLOCK), bf16)
    return pl.pallas_call(
        weight_body,
        grid_spec=pltpu.PrefetchScalarGridSpec(
            num_scalar_prefetch=1,
            grid=(8,),
            in_specs=[HBM] * 4 + [whole_spec((1, D))],
            out_specs=[block, block],
            scratch_shapes=[
                pltpu.VMEM((SEQ, D), bf16),
                pltpu.VMEM((SEQ, WIDTH), bf16),
                pltpu.VMEM((SEQ, QW), bf16),
                pltpu.VMEM((SEQ, D), bf16),
                pltpu.VMEM((SEQ, TILE), f32),
                pltpu.SemaphoreType.DMA((4,)),
            ],
        ),
        out_shape=[shape, shape],
        compiler_params=limit(56),
        name="weight_stage",
    )(at, layer_inputs, proj_grads, attn_stash, out_grads, gain)


def wide(array):
    return array.astype(f32)


def prepare_body(kept, received, up, down, k, r, sems):
    copies = []
    for n in range(2):
        far = (4 * n + 2, pl.ds(0, Q_ROWS))
        copies.append(pltpu.make_async_copy(kept.at[far], k.at[n], sems.at[2 * n]))
        copies.append(pltpu.make_async_copy(received.at[far], r.at[n], sems.at[2 * n + 1]))
    for copy in copies:
        copy.start()
    for copy in copies:
        copy.wait()
    for n, out in enumerate((up, down)):
        out[...] = (wide(k[n]) + wide(r[n])).astype(bf16)


def prepare_stage(kept, received):
    shape = jax.ShapeDtypeStruct((Q_ROWS, BLOCK), bf16)
    return pl.pallas_call(
        prepare_body,
        in_specs=[HBM] * 2,
        out_specs=[VMEM] * 2,
        out_shape=[shape, shape],
        scratch_shapes=[
            pltpu.VMEM((2, Q_ROWS, BLOCK), bf16),
            pltpu.VMEM((2, Q_ROWS, BLOCK), bf16),
            pltpu.SemaphoreType.DMA((4,)),
        ],
        compiler_params=limit(10),
        name="prepare",
    )(kept, received)


def final_body(mine, last, qkv):
    total = mine[...] + last[...].astype(f32)
    for j in range(3):
        qkv[0, :, j * BLOCK : (j + 1) * BLOCK] = total[j * TILE : (j + 1) * TILE]


def final_sum(mine, last):
    return pl.pallas_call(
        final_body,
        in_specs=[VMEM] * 2,
        out_specs=VMEM,
        out_shape=jax.ShapeDtypeStruct((1, TILE, WIDTH), f32),
        compiler_params=limit(6),
        name="final_sum",
    )(mine, last)


def out_body(mine, far, above, below, out):
    total = mine[...] + wide(far[...]) + wide(above[...]) + wide(below[...])
    for j in range(4):
        out[0, :, j * BLOCK : (j + 1) * BLOCK] = total[j * HEAD_DIM : (j + 1) * HEAD_DIM]


def out_total(*arrays):
    return pl.pallas_call(
        out_body,
        in_specs=[VMEM] * 4,
        out_specs=VMEM,
        out_shape=jax.ShapeDtypeStruct((1, HEAD_DIM, D), f32),
        compiler_params=limit(6),
        name="out_total",
    )(*arrays)


def scattered(sent, kept):
    received = passed_along(sent, "core", 1)
    across = (wide(kept[4:, Q_ROWS:]) + wide(received[4:, Q_ROWS:])).astype(bf16)
    across = passed_along(across, "x_hi", 1)
    up, down = prepare_stage(kept, received)
    up = wide(from_below(up))
    down = wide(from_above(down))

    def qkv_sum(dx, dy):
        at = 4 * dx + dy
        return wide(kept[at, :Q_ROWS]) + wide(received[at, :Q_ROWS])

    def out_sum(dy):
        return wide(kept[dy, Q_ROWS:]) + wide(received[dy, Q_ROWS:]) + wide(across[dy])

    above = jnp.concatenate([qkv_sum(0, 1) + up, qkv_sum(1, 1)])
    below = jnp.concatenate([qkv_sum(0, 3), qkv_sum(1, 3) + down])
    above = wide(from_below(above.astype(bf16)))
    below = wide(from_above(below.astype(bf16)))
    out_far = passed_along(out_sum(2).astype(bf16), "y", 2)
    out_above = from_below(out_sum(1).astype(bf16))
    out_below = from_above(out_sum(3).astype(bf16))
    kept_rows = qkv_sum(0, 0) + above[:Q_ROWS] + below[:Q_ROWS]
    sent_rows = qkv_sum(1, 0) + above[Q_ROWS:] + below[Q_ROWS:]
    last = passed_along(sent_rows.astype(bf16), "x_hi", 1)
    return (final_sum(kept_rows, last), out_total(out_sum(0), out_far, out_above, out_below))


def local_step(
    layer_inputs, out_grads, attn_stash, proj_grads, w_qkv, w_out, norm_gain, b_sched, w_sched
):
    tables = rope_tables(SEQ)
    place = [lax.axis_index(name) for name in FSDP]
    at_b = jnp.stack([*place, b_sched[0]]).astype(jnp.int32)
    at_w = jnp.stack([*place, w_sched[0]]).astype(jnp.int32)
    groups = gathered_groups(packed_shard(w_qkv, w_out))
    sent, kept = weight_stage(at_w, layer_inputs, proj_grads, attn_stash, out_grads, norm_gain)
    acc, attn_grad, rest = first_stage(at_b, layer_inputs, out_grads, norm_gain, groups[:2])
    acc, attn_grad = more_stage(at_b, out_grads, acc, attn_grad, rest, groups[2])
    grads = scattered(sent, kept)
    second, *carried = second_stage(
        at_b, layer_inputs, out_grads, norm_gain, tables, acc, attn_grad, rest, groups
    )
    second = passed_along(second, SECTION, -1)
    first = third_stage(at_b, layer_inputs, out_grads, norm_gain, tables, carried, groups)
    first = passed_along(first, SECTION, -1)
    sent_back = jnp.concatenate([first, second], axis=0)
    return (sent_back[None], *grads)


def solution(mesh):
    finer = Mesh(mesh.devices.reshape(mesh.shape["section"] // 2, 2, 2, 4, 2), SECTION + FSDP)
    return jax.shard_map(
        local_step,
        mesh=finer,
        in_specs=(
            P(SECTION, None, FSDP, None),
            P(SECTION, None, FSDP, None),
            P(SECTION, None, FSDP, None),
            P(SECTION, None, FSDP, None),
            P(SECTION, FSDP, None),
            P(SECTION, FSDP, None),
            P(SECTION, None),
            P(SECTION),
            P(SECTION),
        ),
        out_specs=(P(SECTION, FSDP, None), P(SECTION, FSDP, None), P(SECTION, FSDP, None)),
        check_vma=False,
    )
```
